32 devices in a mesh: tp: 8 (over z, y), dp: 4 (over x, core).
Axes of the slice: x: 2, y: 2, z: 4, core: 2. Of those that a mesh axis runs over, the one named last changes fastest.
Arguments:
- hidden: bfloat16 [4, 128, 1024], P('dp')
- ln_gamma: float32 [1024], replicated
- ln_beta: float32 [1024], replicated
- embed_table: bfloat16 [250880, 1024], P('tp')
- labels: int32 [4, 128], P('dp')
- loss_mask: int32 [4, 128], P('dp')
Outputs:
- output 1: float32 [], replicated
- output 2: bfloat16 [4, 128, 1024], P('dp')
- output 3: float32 [250880, 1024], P('tp')
- output 4: float32 [1024], replicated
- output 5: float32 [1024], replicated
All inputs are finite; a program needn't handle non-finite values.
Results may differ from the reference program's by a relative error of at most 0.001.
Values sent between devices are 32-bit elements.
A program may use at most 1 GiB of HBM per device.

```python
import jax
import jax.numpy as jnp
from jax import lax

HIDDEN = 1024
VOCAB_SIZE = 250880
NUM_SEQS = 4
SEQ_LEN = 128
TOKEN_BLOCK = min(SEQ_LEN, 128)
LAYER_EPS = 1e-5
SCORE_SCALE = 3.5


def setup_inputs(seed: int = 0) -> dict:
    rand_keys = jax.random.split(jax.random.key(seed), 6)
    hidden = (1.5 * jax.random.normal(rand_keys[0], (NUM_SEQS, SEQ_LEN, HIDDEN), jnp.float32)).astype(jnp.bfloat16)
    ln_gamma = 1.0 + 0.3 * jax.random.normal(rand_keys[1], (HIDDEN,), jnp.float32)
    ln_beta = 0.3 * jax.random.normal(rand_keys[2], (HIDDEN,), jnp.float32)
    embed_table = (SCORE_SCALE * HIDDEN ** -0.5 * jax.random.normal(rand_keys[3], (VOCAB_SIZE, HIDDEN), jnp.float32)).astype(jnp.bfloat16)
    labels = jax.random.randint(rand_keys[4], (NUM_SEQS, SEQ_LEN), 0, VOCAB_SIZE, jnp.int32)
    lengths = jax.random.randint(rand_keys[5], (NUM_SEQS, 1), 1, SEQ_LEN + 1, jnp.int32)
    positions = jnp.arange(SEQ_LEN, dtype=jnp.int32)[None, :]
    loss_mask = (positions < lengths).astype(jnp.int32)
    return {'hidden': hidden, 'ln_gamma': ln_gamma, 'ln_beta': ln_beta, 'embed_table': embed_table, 'labels': labels, 'loss_mask': loss_mask}


def reference(hidden, ln_gamma, ln_beta, embed_table, labels, loss_mask):
    mask_float = loss_mask.astype(jnp.float32)
    token_count = jnp.sum(mask_float)
    vocab_ids = jnp.arange(VOCAB_SIZE, dtype=jnp.int32)[None, :]
    block_hidden = hidden.reshape(-1, TOKEN_BLOCK, HIDDEN)
    block_labels = labels.reshape(-1, TOKEN_BLOCK)
    block_mask = mask_float.reshape(-1, TOKEN_BLOCK, 1)

    def block_step(scan_carry, block_data):
        d_embed, d_gamma, d_beta, loss_sum = scan_carry
        block_rows, row_labels, row_mask = block_data
        x_float = block_rows.astype(jnp.float32)
        row_mean = jnp.mean(x_float, axis=-1, keepdims=True)
        centered = x_float - row_mean
        inv_std = lax.rsqrt(jnp.mean(centered * centered, axis=-1, keepdims=True) + LAYER_EPS)
        x_hat = centered * inv_std
        normed = (x_hat * ln_gamma + ln_beta).astype(jnp.bfloat16)
        logits = jnp.dot(normed, embed_table.T, preferred_element_type=jnp.float32)
        row_max = jnp.max(logits, axis=-1, keepdims=True)
        log_norm = row_max + jnp.log(jnp.sum(jnp.exp(logits - row_max), axis=-1, keepdims=True))
        is_target = vocab_ids == row_labels[:, None]
        target_logit = jnp.sum(jnp.where(is_target, logits, 0.0), axis=-1, keepdims=True)
        loss_sum = loss_sum + jnp.sum(row_mask * (log_norm - target_logit))
        soft_probs = jnp.exp(logits - log_norm)
        grad_logits = (jnp.where(is_target, soft_probs - 1.0, soft_probs) * (row_mask / token_count)).astype(jnp.bfloat16)
        grad_normed = jnp.dot(grad_logits, embed_table, preferred_element_type=jnp.float32)
        d_embed = d_embed + jnp.dot(grad_logits.T, normed, preferred_element_type=jnp.float32)
        d_gamma = d_gamma + jnp.sum(grad_normed * x_hat, axis=0)
        d_beta = d_beta + jnp.sum(grad_normed, axis=0)
        grad_scaled = grad_normed * ln_gamma
        grad_x = (grad_scaled - jnp.mean(grad_scaled, axis=-1, keepdims=True) - x_hat * jnp.mean(grad_scaled * x_hat, axis=-1, keepdims=True)) * inv_std
        return (d_embed, d_gamma, d_beta, loss_sum), grad_x.astype(jnp.bfloat16)

    zero_carry = (jnp.zeros((VOCAB_SIZE, HIDDEN), jnp.float32), jnp.zeros((HIDDEN,), jnp.float32), jnp.zeros((HIDDEN,), jnp.float32), jnp.zeros((), jnp.float32))
    final_carry, grad_blocks = lax.scan(block_step, zero_carry, (block_hidden, block_labels, block_mask))
    d_embed, d_gamma, d_beta, loss_sum = final_carry
    d_hidden = grad_blocks.reshape(NUM_SEQS, SEQ_LEN, HIDDEN)
    return loss_sum / token_count, d_hidden, d_embed, d_gamma, d_beta
```

```python
import functools

import jax
import jax.numpy as jnp
from jax import lax
from jax.experimental import pallas as pl
from jax.experimental.pallas import tpu as pltpu
from jax.sharding import PartitionSpec as P

MESH = pl.DeviceIdType.MESH
LAYER_EPS = 1e-5
SEQ = 128
BLOCK = 256
IN_SLOTS = 3


def dot(a, b, contract, precision=None):
    return lax.dot_general(a, b, ((contract[0], contract[1]), ((), ())), precision=precision, preferred_element_type=jnp.float32)


def layer_norm(h, gamma, beta):
    centered = h - jnp.mean(h, axis=-1, keepdims=True)
    inv_std = lax.rsqrt(jnp.mean(centered * centered, axis=-1, keepdims=True) + LAYER_EPS)
    x_hat = centered * inv_std
    return x_hat, inv_std, (x_hat * gamma + beta).astype(jnp.bfloat16)


def front_kernel(n_tp, rows, tile, hid_ref, gamma_ref, beta_ref, lab_ref, mask_ref, embed_ref,
                 half_ref, zc_ref, zt_ref, hw_ref, wmask_ref, stats_ref, pos_ref,
                 hx, z_all, h_chip, logit, st, e_sem, x_send, x_recv, st_send, st_recv):
    tp, dp = lax.axis_index('tp'), lax.axis_index('dp')
    n_dev = n_tp * 4
    me = tp * 4 + dp
    x, c = dp // 2, dp % 2
    sib, far = x * 2 + (1 - c), (1 - x) * 2 + c
    far_sib = (1 - x) * 2 + (1 - c)
    half = rows // 2
    tiles = half // tile
    width = hid_ref.shape[1]

    def fetch(i):
        return pltpu.make_async_copy(
            embed_ref.at[pl.ds(pl.multiple_of(c * half + i * tile, 16), tile)],
            half_ref.at[pl.ds(pl.multiple_of(i * tile, 16), tile)], e_sem.at[i])

    def start_fetch(i, carry):
        fetch(i).start()
        return carry

    lax.fori_loop(0, tiles, start_fetch, 0)

    barrier = pltpu.get_barrier_semaphore()

    def hello(k, carry):
        peer = lax.rem(me + k, n_dev)
        pl.semaphore_signal(barrier, inc=1, device_id=(peer // 4, lax.rem(peer, 4)), device_id_type=MESH)
        return carry

    lax.fori_loop(1, n_dev, hello, 0)

    lab = jnp.broadcast_to(lab_ref[...].astype(jnp.float32), (8, SEQ))
    msk = jnp.broadcast_to(mask_ref[...].astype(jnp.float32), (8, SEQ))
    hx[dp, pl.ds(SEQ, 8), :] = jnp.concatenate([lab, msk, jnp.zeros((8, width - 2 * SEQ), jnp.float32)], axis=1)

    def widen(r, carry):
        at = pl.ds(pl.multiple_of(r * 32, 32), 32)
        hx[dp, at, :] = hid_ref[at, :].astype(jnp.float32)
        return carry

    lax.fori_loop(0, SEQ // 32, widen, 0)

    def norm(slot):
        def chunk(r, carry):
            at = pl.multiple_of(r * 32, 32)
            h = hx[slot, pl.ds(at, 32), :]
            z_all[pl.ds(pl.multiple_of(slot * SEQ + at, 32), 32), :] = layer_norm(h, gamma_ref[...], beta_ref[...])[2]
            return carry
        lax.fori_loop(0, SEQ // 32, chunk, 0)

    def chip_rows(slot, place):
        def chunk(r, carry):
            at = pl.multiple_of(r * 32, 32)
            h_chip[pl.ds(pl.multiple_of(place * SEQ + at, 32), 32), :] = hx[slot, pl.ds(at, 32), :].astype(jnp.bfloat16)
            return carry
        lax.fori_loop(0, SEQ // 32, chunk, 0)

    norm(dp)
    chip_rows(dp, c)
    pl.semaphore_wait(barrier, n_dev - 1)

    def send(slot, k, to):
        return pltpu.make_async_remote_copy(
            src_ref=hx.at[slot], dst_ref=hx.at[slot], send_sem=x_send.at[k], recv_sem=x_recv.at[k],
            device_id=(tp, to), device_id_type=MESH)

    to_sib, to_far = send(dp, 0, sib), send(dp, 1, far)
    to_far.start()
    to_sib.start()
    send(sib, 0, sib).wait_recv()
    norm(sib)
    chip_rows(sib, 1 - c)

    def labels_of(slot):
        return hx[slot, pl.ds(SEQ, 1), pl.ds(0, SEQ)]

    chip_lab = jnp.concatenate([labels_of(2 * x), labels_of(2 * x + 1)], axis=1).astype(jnp.int32)
    first_row = tp * rows + c * half
    chip_tokens = pl.ds(pl.multiple_of(x * BLOCK, BLOCK), BLOCK)
    piece = tile // 14 if tile % (14 * 8) == 0 else tile

    def product(i):
        logit[...] = dot(half_ref[pl.ds(pl.multiple_of(i * tile, 16), tile), :], z_all[chip_tokens, :], ((1,), (1,)))

    fetch(0).wait()
    product(0)
    row_iota = lax.broadcasted_iota(jnp.int32, (piece, BLOCK), 0)

    def body(i, carry):
        top, total, target = carry
        later = jnp.minimum(i + 1, tiles - 1)

        @pl.when(i + 1 < tiles)
        def _():
            fetch(i + 1).wait()

        new_top = top
        for r in range(0, tile, piece):
            v = logit[pl.ds(r, piece), :].reshape(piece // 8, 8, BLOCK)
            new_top = jnp.maximum(new_top, jnp.max(v, axis=0))
        total = total * jnp.exp(top - new_top)
        lab_here = chip_lab - (first_row + i * tile)
        for r in range(0, tile, piece):
            v = logit[pl.ds(r, piece), :]
            e = jnp.exp(v.reshape(piece // 8, 8, BLOCK) - new_top[None])
            total = total + jnp.sum(e, axis=0)
            hit = jnp.where(row_iota == lab_here - r, v, 0.0)
            target = target + jnp.sum(hit.reshape(piece // 8, 8, BLOCK), axis=0)
        product(later)
        return new_top, total, target

    start = (jnp.full((8, BLOCK), -jnp.inf, jnp.float32), jnp.zeros((8, BLOCK), jnp.float32), jnp.zeros((8, BLOCK), jnp.float32))
    first = jnp.max(logit[...].reshape(tile // 8, 8, BLOCK), axis=0)
    top, total, target = lax.fori_loop(0, tiles, body, (first, start[1], start[2]))

    best = jnp.max(top, axis=0, keepdims=True)
    part = best + jnp.log(jnp.sum(total * jnp.exp(top - best), axis=0, keepdims=True))
    st[me, pl.ds(0, 1), :] = part
    st[me, pl.ds(1, 1), :] = jnp.sum(target, axis=0, keepdims=True)

    def stat(k, owner):
        peer = lax.rem(me + k, n_dev)
        return pltpu.make_async_remote_copy(
            src_ref=st.at[me], dst_ref=st.at[owner], send_sem=st_send.at[k], recv_sem=st_recv.at[owner],
            device_id=(peer // 4, lax.rem(peer, 4)), device_id_type=MESH)

    def send_stat(k, carry):
        stat(k, me).start()
        return carry

    lax.fori_loop(1, n_dev, send_stat, 0)

    send(far, 1, far).wait_recv()
    to_sib2 = send(far, 2, sib)
    to_sib2.start()
    norm(far)
    send(far_sib, 2, sib).wait_recv()
    norm(far_sib)

    lab_all = jnp.concatenate([labels_of(s) for s in range(4)], axis=1)
    mask_all = jnp.concatenate([hx[s, pl.ds(SEQ, 1), pl.ds(SEQ, SEQ)] for s in range(4)], axis=1)
    n_tok = 4 * SEQ
    lane = lax.broadcasted_iota(jnp.int32, (1, n_tok), 1)
    up = lax.broadcasted_iota(jnp.int32, (n_tok, n_tok), 0)
    across = lax.broadcasted_iota(jnp.int32, (n_tok, n_tok), 1)
    before = jnp.where((up < across) & (up // BLOCK == across // BLOCK), 1.0, 0.0).astype(jnp.bfloat16)
    rank = dot(jnp.broadcast_to(mask_all, (8, n_tok)).astype(jnp.bfloat16), before, ((1,), (0,)))[0:1, :]
    count_0 = jnp.sum(mask_all[:, :BLOCK], axis=1, keepdims=True)
    count_1 = jnp.sum(mask_all[:, BLOCK:], axis=1, keepdims=True)
    count = count_0 + count_1
    one_block = count <= BLOCK
    base_1 = jnp.where(one_block, BLOCK, 2 * BLOCK) - count_1
    col = jnp.where(lane < BLOCK, rank, rank + base_1)
    col = jnp.where(mask_all > 0.0, col, -1.0).astype(jnp.int32)
    chosen = up == col
    packing = jnp.where(chosen, 1.0, 0.0)
    packing_16 = packing.astype(jnp.bfloat16)
    zc_ref[...] = dot(packing_16, z_all[...], ((1,), (0,))).astype(jnp.bfloat16)
    zt_ref[...] = dot(z_all[...], packing_16, ((0,), (1,))).astype(jnp.bfloat16)

    window = jnp.where(one_block, 0, x * BLOCK)
    mine = jnp.where(x == 0, col[:, :BLOCK], col[:, BLOCK:]) - window
    w_pack = jnp.where(lax.broadcasted_iota(jnp.int32, (BLOCK, BLOCK), 0) == mine, 1.0, 0.0)
    hw_ref[...] = dot(w_pack.astype(jnp.bfloat16), h_chip[...], ((1,), (0,))).astype(jnp.bfloat16)
    wmask_ref[...] = jnp.broadcast_to(jnp.sum(w_pack, axis=1, keepdims=True), (BLOCK, 128))
    own = jnp.where(c == 0, mine[:, :SEQ], mine[:, SEQ:])
    pos_ref[...] = jnp.broadcast_to(own, (8, SEQ))

    def wait_stat(k, carry):
        stat(k, lax.rem(me + k, n_dev)).wait_recv()
        return carry

    lax.fori_loop(1, n_dev, wait_stat, 0)
    lse, goal = [], []
    for group in range(2):
        ids = [t * 4 + 2 * group + k for t in range(n_tp) for k in range(2)]
        parts = [st[d, pl.ds(0, 1), :] for d in ids]
        m = functools.reduce(jnp.maximum, parts)
        lse.append(m + jnp.log(sum(jnp.exp(p - m) for p in parts)))
        goal.append(sum(st[d, pl.ds(1, 1), :] for d in ids))
    lse, goal = jnp.concatenate(lse, axis=1), jnp.concatenate(goal, axis=1)
    loss = jnp.sum(mask_all * (lse - goal), axis=1, keepdims=True) / count

    values = jnp.concatenate([lse, lab_all, jnp.ones((6, n_tok), jnp.float32)], axis=0)
    packed = dot(values, packing, ((1,), (1,)), lax.Precision.HIGHEST)
    used = jnp.sum(jnp.where(packed[2:3, :] > 0.5, 1.0, 0.0), axis=0, keepdims=True)
    stats_ref[pl.ds(0, 1), :] = jnp.where(used > 0.5, packed[0:1, :], 1e30)
    stats_ref[pl.ds(1, 1), :] = jnp.where(used > 0.5, packed[1:2, :], -1.0)
    stats_ref[pl.ds(2, 1), :] = jnp.broadcast_to(1.0 / count, (1, n_tok))
    stats_ref[pl.ds(3, 1), :] = jnp.broadcast_to(count, (1, n_tok))
    stats_ref[pl.ds(4, 1), :] = jnp.broadcast_to(loss, (1, n_tok))
    stats_ref[pl.ds(5, 3), :] = jnp.zeros((3, n_tok), jnp.float32)

    to_sib.wait_send()
    to_far.wait_send()
    to_sib2.wait_send()

    def wait_sent(k, carry):
        stat(k, me).wait_send()
        return carry

    lax.fori_loop(1, n_dev, wait_sent, 0)


def back_kernel(tile, resident, slots, t_0, t_1, *refs):
    if resident:
        embed_ref, zc_ref, zt_ref, stats_ref, out_ref, dz_ref, logit, grad, staged, out_sem = refs
    else:
        embed_ref, zc_ref, zt_ref, stats_ref, _, out_ref, logit, grad, staged, out_sem, held, in_sem = refs
    tp, dp = lax.axis_index('tp'), lax.axis_index('dp')
    chip, c = dp // 2, dp % 2
    rows = out_ref.shape[0]
    vocab_0, row_0 = tp * rows, (c if resident else 1 - c) * (rows // 2)
    count = jnp.max(stats_ref[pl.ds(3, 1), :])
    chunk = tile // 5 if tile % (5 * 16) == 0 else tile
    piece = chunk // 2 if chunk % 32 == 0 else chunk
    width = zc_ref.shape[1]

    def fetch(i):
        slot = lax.rem(i, IN_SLOTS)
        return pltpu.make_async_copy(embed_ref.at[pl.ds(pl.multiple_of(row_0 + i * tile, 16), tile)], held.at[slot], in_sem.at[slot])

    def rows_of(i, r, n):
        if resident:
            return embed_ref[pl.ds(pl.multiple_of(i * tile + r, 16), n), :]
        return held[lax.rem(i, IN_SLOTS), pl.ds(r, n), :]

    def put(i):
        slot = lax.rem(i, slots)
        return pltpu.make_async_copy(staged.at[slot], out_ref.at[pl.ds(pl.multiple_of(row_0 + i * tile, 16), tile)], out_sem.at[slot])

    def run(blocks):
        cols = blocks * BLOCK
        lse = stats_ref[pl.ds(0, 1), pl.ds(0, cols)]
        label = stats_ref[pl.ds(1, 1), pl.ds(0, cols)].astype(jnp.int32) - (vocab_0 + row_0)
        scale = stats_ref[pl.ds(2, 1), pl.ds(0, cols)]
        row_iota = lax.broadcasted_iota(jnp.int32, (piece, cols), 0)

        def product(i, r):
            logit[pl.ds(r, chunk), pl.ds(0, cols)] = dot(rows_of(i, r, chunk), zt_ref[:, pl.ds(0, cols)], ((1,), (0,)))

        if not resident:
            for k in range(IN_SLOTS - 1):
                if t_0 + k < t_1:
                    fetch(t_0 + k).start()
            fetch(t_0).wait()
        else:
            dz_ref[...] = jnp.zeros_like(dz_ref)
        for r in range(0, tile, chunk):
            product(t_0, r)

        def body(i, carry):
            later = jnp.minimum(i + 1, t_1 - 1)
            if not resident:
                @pl.when(i + IN_SLOTS - 1 < t_1)
                def _():
                    fetch(i + IN_SLOTS - 1).start()

                @pl.when(i + 1 < t_1)
                def _():
                    fetch(i + 1).wait()

            @pl.when(i - slots >= t_0)
            def _():
                put(i - slots).wait()

            here = label - i * tile
            for q in range(0, tile, chunk):
                for r in range(q, q + chunk, piece):
                    p = jnp.exp(logit[pl.ds(r, piece), pl.ds(0, cols)] - lse)
                    g = jnp.where(row_iota == here - r, p - 1.0, p) * scale
                    grad[pl.ds(r, piece), pl.ds(0, cols)] = g.astype(jnp.bfloat16)
                product(later, q)
                staged[lax.rem(i, slots), pl.ds(q, chunk), :] = dot(grad[pl.ds(q, chunk), pl.ds(0, cols)], zc_ref[pl.ds(0, cols), :], ((1,), (0,)))
            if resident:
                window = grad[:, pl.ds(0, BLOCK)]
                if blocks > 1:
                    window = jnp.where(chip == 0, window, grad[:, pl.ds(BLOCK, BLOCK)])
                for n in range(0, width, 256):
                    dz_ref[:, pl.ds(n, 256)] += dot(window, rows_of(i, 0, tile)[:, n:n + 256], ((0,), (0,)))
            put(i).start()
            return carry

        lax.fori_loop(t_0, t_1, body, 0)

        def drain(i, carry):
            put(i).wait()
            return carry

        lax.fori_loop(max(t_0, t_1 - slots), t_1, drain, 0)

    @pl.when(count <= BLOCK)
    def _():
        run(1)

    @pl.when(count > BLOCK)
    def _():
        run(2)


def deal_kernel(n_tp, dz_ref, arrived_ref, *part_refs):
    share = part_refs[0].shape[0]
    for k in range(n_tp):
        owner = lax.rem(lax.axis_index('tp') + k, n_tp)
        at = pl.multiple_of(owner * share, 8)
        mine = dz_ref[pl.ds(pl.multiple_of(lax.rem(lax.axis_index('dp'), 2) * (n_tp * share) + at, 8), share), :]
        part_refs[k][...] = mine + arrived_ref[pl.ds(at, share), :]


def norm_kernel(n_tp, hw_ref, wmask_ref, gamma_ref, beta_ref, *refs):
    got, packet_ref = refs[:-1], refs[-1]
    share, width = got[0].shape
    dz = functools.reduce(jnp.add, [g[...] for g in got])
    at = pl.multiple_of(lax.rem(lax.axis_index('dp'), 2) * (n_tp * share) + lax.axis_index('tp') * share, 8)
    gamma = gamma_ref[...]
    x_hat, inv_std, _ = layer_norm(hw_ref[pl.ds(at, share), :].astype(jnp.float32), gamma, beta_ref[...])
    scaled = dz * gamma
    packet_ref[pl.ds(0, share), :] = (
        scaled - jnp.mean(scaled, axis=-1, keepdims=True) - x_hat * jnp.mean(scaled * x_hat, axis=-1, keepdims=True)) * inv_std
    kept = dz * wmask_ref[pl.ds(at, share), pl.ds(0, 1)]
    d_gamma = jnp.sum(kept * x_hat, axis=0, keepdims=True)
    d_beta = jnp.sum(kept, axis=0, keepdims=True)
    row = lax.broadcasted_iota(jnp.int32, (8, width), 0)
    packet_ref[pl.ds(share, 8), :] = jnp.where(row == 0, d_gamma, jnp.where(row == 1, d_beta, 0.0))


def order_kernel(n_tp, *refs):
    packets, (win_ref, sums_ref) = refs[:n_tp], refs[n_tp:n_tp + 2]
    share = packets[0].shape[0] - 8
    for k in range(n_tp):
        owner = lax.rem(lax.axis_index('tp') + k, n_tp)
        win_ref[pl.ds(pl.multiple_of(owner * share, 8), share), :] = packets[k][pl.ds(0, share), :]
    total = jnp.zeros_like(sums_ref)
    for owner in range(n_tp):
        term = packets[0][pl.ds(share, 8), :]
        for k in range(1, n_tp):
            term = jnp.where(lax.rem(lax.axis_index('tp') + k, n_tp) == owner, packets[k][pl.ds(share, 8), :], term)
        total = total + term
    sums_ref[...] = total


def finish_kernel(pos_ref, win_ref, other_ref, *refs):
    per_dp, (hidden_ref, gamma_ref, beta_ref) = refs[:4], refs[4:]
    total = jnp.zeros_like(per_dp[0])
    for owner in range(4):
        term = per_dp[0][...]
        for k in range(1, 4):
            term = jnp.where(lax.rem(lax.axis_index('dp') + k, 4) == owner, per_dp[k][...], term)
        total = total + term
    gamma_ref[...] = total[0:1, :]
    beta_ref[...] = total[1:2, :]
    lower = win_ref.shape[0]
    slot = pos_ref[0:1, :] - lax.rem(lax.axis_index('dp'), 2) * lower
    slot = jnp.where(slot < 0, slot + 2 * lower, slot)
    slot = jnp.where(pos_ref[0:1, :] < 0, -1, slot)
    up = lax.broadcasted_iota(jnp.int32, (lower, slot.shape[1]), 0)
    out = jnp.zeros(hidden_ref.shape, jnp.float32)
    for part, ref in enumerate((win_ref, other_ref)):
        pick = jnp.where(up + part * lower == slot, 1.0, 0.0).astype(jnp.bfloat16)
        out = out + dot(pick, ref[...].astype(jnp.bfloat16), ((0,), (0,)))
    hidden_ref[...] = out.astype(jnp.bfloat16)


VMEM = pl.BlockSpec(memory_space=pltpu.VMEM)
ANY = pl.BlockSpec(memory_space=pl.ANY)


def solution(mesh):
    n_tp, n_dp = mesh.shape['tp'], mesh.shape['dp']

    def local_step(hidden, ln_gamma, ln_beta, embed, labels, loss_mask):
        tp, dp = lax.axis_index('tp'), lax.axis_index('dp')
        rows, width = embed.shape
        half = rows // 2
        tile = 1120 if half % 1120 == 0 else half // 7
        tiles = half // tile
        x, c = dp // 2, dp % 2
        f32, bf16 = jnp.float32, jnp.bfloat16

        e_half, zc, zt, hw, wmask, stats, pos = pl.pallas_call(
            functools.partial(front_kernel, n_tp, rows, tile),
            out_shape=(pltpu.VMEM((half, width), bf16), jax.ShapeDtypeStruct((4 * SEQ, width), bf16), jax.ShapeDtypeStruct((width, 4 * SEQ), bf16),
                       jax.ShapeDtypeStruct((BLOCK, width), bf16), jax.ShapeDtypeStruct((BLOCK, 128), f32),
                       jax.ShapeDtypeStruct((8, 4 * SEQ), f32), jax.ShapeDtypeStruct((8, SEQ), jnp.int32)),
            in_specs=[VMEM] * 5 + [ANY],
            out_specs=[VMEM] * 7,
            scratch_shapes=[
                pltpu.VMEM((4, SEQ + 8, width), f32), pltpu.VMEM((4 * SEQ, width), bf16), pltpu.VMEM((BLOCK, width), bf16),
                pltpu.VMEM((tile, BLOCK), f32), pltpu.VMEM((4 * n_tp, 2, BLOCK), f32),
                pltpu.SemaphoreType.DMA((tiles,)), pltpu.SemaphoreType.DMA((3,)), pltpu.SemaphoreType.DMA((3,)),
                pltpu.SemaphoreType.DMA((4 * n_tp,)), pltpu.SemaphoreType.DMA((4 * n_tp,)),
            ],
            compiler_params=pltpu.CompilerParams(collective_id=0, has_side_effects=True, vmem_limit_bytes=12 << 20),
            cost_estimate=pl.CostEstimate(flops=2 * half * BLOCK * width, bytes_accessed=2 * half * width, transcendentals=0),
        )(hidden[0], ln_gamma[None], ln_beta[None], labels, loss_mask, embed)

        def back(resident, source, t_0, t_1, d_embed=None):
            slots = 2 if resident else 3
            scratch = [pltpu.VMEM((tile, 2 * BLOCK), f32), pltpu.VMEM((tile, 2 * BLOCK), bf16),
                       pltpu.VMEM((slots, tile, width), f32), pltpu.SemaphoreType.DMA((slots,))]
            ops, specs = [source, zc, zt, stats], [VMEM if resident else ANY, VMEM, VMEM, VMEM]
            shapes, outs, alias = [jax.ShapeDtypeStruct((rows, width), f32)], [ANY], {}
            if resident:
                shapes.append(jax.ShapeDtypeStruct((BLOCK, width), f32))
                outs.append(VMEM)
            else:
                ops.append(d_embed)
                specs.append(ANY)
                alias = {4: 0}
                scratch += [pltpu.VMEM((IN_SLOTS, tile, width), bf16), pltpu.SemaphoreType.DMA((IN_SLOTS,))]
            n = t_1 - t_0
            return pl.pallas_call(
                functools.partial(back_kernel, tile, resident, slots, t_0, t_1), out_shape=shapes, in_specs=specs, out_specs=outs,
                scratch_shapes=scratch, input_output_aliases=alias,
                compiler_params=pltpu.CompilerParams(vmem_limit_bytes=(16 if resident else 34) << 20, has_side_effects=True),
                cost_estimate=pl.CostEstimate(flops=6 * n * tile * BLOCK * width, bytes_accessed=6 * n * tile * width, transcendentals=0),
            )(*ops)

        d_embed, dz = back(True, e_half, 0, tiles)

        def small(body, out_shape, *ops):
            return pl.pallas_call(
                body, out_shape=out_shape, in_specs=[VMEM] * len(ops), out_specs=jax.tree.map(lambda _: VMEM, out_shape),
                compiler_params=pltpu.CompilerParams(vmem_limit_bytes=8 << 20),
                cost_estimate=pl.CostEstimate(flops=1 << 20, bytes_accessed=1 << 20, transcendentals=0),
            )(*ops)

        cuts = [0, tiles // 7, tiles // 2, tiles * 6 // 7, tiles]

        def shape(*dims):
            return jax.ShapeDtypeStruct(dims, f32)

        lower = BLOCK // 2
        share = lower // n_tp
        swap = [(0, 1), (1, 0), (2, 3), (3, 2)]
        arrived = lax.ppermute(lax.dynamic_slice_in_dim(dz, (1 - c) * lower, lower, 0), 'dp', swap)
        (d_embed,) = back(False, embed, cuts[0], cuts[1], d_embed)

        parts = list(small(functools.partial(deal_kernel, n_tp), [shape(share, width)] * n_tp, dz, arrived))
        got = [parts[0]] + [lax.ppermute(parts[k], 'tp', [(i, (i + k) % n_tp) for i in range(n_tp)]) for k in range(1, n_tp)]
        d_embed, parts[0] = lax.optimization_barrier((d_embed, parts[0]))
        (d_embed,) = back(False, embed, cuts[1], cuts[2], d_embed)

        packet = small(functools.partial(norm_kernel, n_tp), shape(share + 8, width), hw, wmask, ln_gamma[None], ln_beta[None], *got)
        packets = [packet] + [lax.ppermute(packet, 'tp', [(i, (i - k) % n_tp) for i in range(n_tp)]) for k in range(1, n_tp)]
        d_embed, packet = lax.optimization_barrier((d_embed, packet))
        (d_embed,) = back(False, embed, cuts[2], cuts[3], d_embed)

        d_win, sums = small(functools.partial(order_kernel, n_tp), [shape(lower, width), shape(8, width)], *packets)
        other = lax.ppermute(d_win, 'dp', swap)
        per_dp = [sums] + [lax.ppermute(sums, 'dp', [(i, (i - k) % n_dp) for i in range(n_dp)]) for k in range(1, n_dp)]
        d_embed, sums = lax.optimization_barrier((d_embed, sums))
        (d_embed,) = back(False, embed, cuts[3], cuts[4], d_embed)
        d_hidden, d_gamma, d_beta = small(
            finish_kernel, [jax.ShapeDtypeStruct((SEQ, width), bf16), shape(1, width), shape(1, width)], pos, d_win, other, *per_dp)
        return stats[4, 0], d_hidden[None], d_embed, d_gamma[0], d_beta[0]

    return jax.shard_map(local_step, mesh=mesh, in_specs=(P('dp', None, None), P(None), P(None), P('tp', None), P('dp', None), P('dp', None)), out_specs=(P(), P('dp', None, None), P('tp', None), P(None), P(None)), check_vma=False)
```

```python
import functools

import jax
import jax.numpy as jnp
from jax import lax
from jax.experimental import pallas as pl
from jax.experimental.pallas import tpu as pltpu
from jax.sharding import PartitionSpec as P

MESH = pl.DeviceIdType.MESH
LAYER_EPS = 1e-5
SEQ = 128
BLOCK = 256
IN_SLOTS = 3


def dot(a, b, contract, precision=None):
    return lax.dot_general(a, b, ((contract[0], contract[1]), ((), ())), precision=precision, preferred_element_type=jnp.float32)


def layer_norm(h, gamma, beta):
    centered = h - jnp.mean(h, axis=-1, keepdims=True)
    inv_std = lax.rsqrt(jnp.mean(centered * centered, axis=-1, keepdims=True) + LAYER_EPS)
    x_hat = centered * inv_std
    return x_hat, inv_std, (x_hat * gamma + beta).astype(jnp.bfloat16)


def front_kernel(n_tp, rows, tile, hid_in, gamma_in, beta_in, lab_in, mask_in, embed_ref,
                 half_ref, zc_ref, zt_ref, hw_ref, wmask_ref, stats_ref, pos_ref,
                 hid_ref, gamma_ref, beta_ref, lab_ref, mask_ref, hx, z_all, h_chip, logit, st, in_sem, e_sem, x_send, x_recv, st_send, st_recv):
    tp, dp = lax.axis_index('tp'), lax.axis_index('dp')
    n_dev = n_tp * 4
    me = tp * 4 + dp
    x, c = dp // 2, dp % 2
    sib, far = x * 2 + (1 - c), (1 - x) * 2 + c
    far_sib = (1 - x) * 2 + (1 - c)
    half = rows // 2
    tiles = half // tile
    width = hid_ref.shape[1]
    pairs = ((hid_in, hid_ref), (gamma_in, gamma_ref), (beta_in, beta_ref), (lab_in, lab_ref), (mask_in, mask_ref))
    loads = [pltpu.make_async_copy(a, b, in_sem.at[k]) for k, (a, b) in enumerate(pairs)]
    for load in loads:
        load.start()

    def fetch(i):
        return pltpu.make_async_copy(
            embed_ref.at[pl.ds(pl.multiple_of(c * half + i * tile, 16), tile)],
            half_ref.at[pl.ds(pl.multiple_of(i * tile, 16), tile)], e_sem.at[i])

    def start_fetch(i, carry):
        fetch(i).start()
        return carry

    lax.fori_loop(0, tiles, start_fetch, 0)

    barrier = pltpu.get_barrier_semaphore()

    def hello(k, carry):
        peer = lax.rem(me + k, n_dev)
        pl.semaphore_signal(barrier, inc=1, device_id=(peer // 4, lax.rem(peer, 4)), device_id_type=MESH)
        return carry

    lax.fori_loop(1, n_dev, hello, 0)

    for load in loads:
        load.wait()
    lab = jnp.broadcast_to(lab_ref[...].astype(jnp.float32), (8, SEQ))
    msk = jnp.broadcast_to(mask_ref[...].astype(jnp.float32), (8, SEQ))
    hx[dp, pl.ds(SEQ, 8), :] = jnp.concatenate([lab, msk, jnp.zeros((8, width - 2 * SEQ), jnp.float32)], axis=1)

    def widen(r, carry):
        at = pl.ds(pl.multiple_of(r * 32, 32), 32)
        hx[dp, at, :] = hid_ref[at, :].astype(jnp.float32)
        return carry

    lax.fori_loop(0, SEQ // 32, widen, 0)

    def norm(slot):
        def chunk(r, carry):
            at = pl.multiple_of(r * 32, 32)
            h = hx[slot, pl.ds(at, 32), :]
            z_all[pl.ds(pl.multiple_of(slot * SEQ + at, 32), 32), :] = layer_norm(h, gamma_ref[...], beta_ref[...])[2]
            return carry
        lax.fori_loop(0, SEQ // 32, chunk, 0)

    def chip_rows(slot, place):
        def chunk(r, carry):
            at = pl.multiple_of(r * 32, 32)
            h_chip[pl.ds(pl.multiple_of(place * SEQ + at, 32), 32), :] = hx[slot, pl.ds(at, 32), :].astype(jnp.bfloat16)
            return carry
        lax.fori_loop(0, SEQ // 32, chunk, 0)

    norm(dp)
    chip_rows(dp, c)
    pl.semaphore_wait(barrier, n_dev - 1)

    def send(slot, k, to):
        return pltpu.make_async_remote_copy(
            src_ref=hx.at[slot], dst_ref=hx.at[slot], send_sem=x_send.at[k], recv_sem=x_recv.at[k],
            device_id=(tp, to), device_id_type=MESH)

    to_sib, to_far = send(dp, 0, sib), send(dp, 1, far)
    to_far.start()
    to_sib.start()
    send(sib, 0, sib).wait_recv()
    norm(sib)
    chip_rows(sib, 1 - c)

    def labels_of(slot):
        return hx[slot, pl.ds(SEQ, 1), pl.ds(0, SEQ)]

    chip_lab = jnp.concatenate([labels_of(2 * x), labels_of(2 * x + 1)], axis=1).astype(jnp.int32)
    first_row = tp * rows + c * half
    chip_tokens = pl.ds(pl.multiple_of(x * BLOCK, BLOCK), BLOCK)
    piece = tile // 14 if tile % (14 * 8) == 0 else tile

    def product(i):
        logit[...] = dot(half_ref[pl.ds(pl.multiple_of(i * tile, 16), tile), :], z_all[chip_tokens, :], ((1,), (1,)))

    fetch(0).wait()
    product(0)
    row_iota = lax.broadcasted_iota(jnp.int32, (piece, BLOCK), 0)

    def body(i, carry):
        top, total, target = carry
        later = jnp.minimum(i + 1, tiles - 1)

        @pl.when(i + 1 < tiles)
        def _():
            fetch(i + 1).wait()

        new_top = top
        for r in range(0, tile, piece):
            v = logit[pl.ds(r, piece), :].reshape(piece // 8, 8, BLOCK)
            new_top = jnp.maximum(new_top, jnp.max(v, axis=0))
        total = total * jnp.exp(top - new_top)
        lab_here = chip_lab - (first_row + i * tile)
        for r in range(0, tile, piece):
            v = logit[pl.ds(r, piece), :]
            e = jnp.exp(v.reshape(piece // 8, 8, BLOCK) - new_top[None])
            total = total + jnp.sum(e, axis=0)
            hit = jnp.where(row_iota == lab_here - r, v, 0.0)
            target = target + jnp.sum(hit.reshape(piece // 8, 8, BLOCK), axis=0)
        product(later)
        return new_top, total, target

    start = (jnp.full((8, BLOCK), -jnp.inf, jnp.float32), jnp.zeros((8, BLOCK), jnp.float32), jnp.zeros((8, BLOCK), jnp.float32))
    first = jnp.max(logit[...].reshape(tile // 8, 8, BLOCK), axis=0)
    top, total, target = lax.fori_loop(0, tiles, body, (first, start[1], start[2]))

    best = jnp.max(top, axis=0, keepdims=True)
    part = best + jnp.log(jnp.sum(total * jnp.exp(top - best), axis=0, keepdims=True))
    st[me, pl.ds(0, 1), :] = part
    st[me, pl.ds(1, 1), :] = jnp.sum(target, axis=0, keepdims=True)

    def stat(k, owner):
        peer = lax.rem(me + k, n_dev)
        return pltpu.make_async_remote_copy(
            src_ref=st.at[me], dst_ref=st.at[owner], send_sem=st_send.at[k], recv_sem=st_recv.at[owner],
            device_id=(peer // 4, lax.rem(peer, 4)), device_id_type=MESH)

    def send_stat(k, carry):
        stat(k, me).start()
        return carry

    lax.fori_loop(1, n_dev, send_stat, 0)

    send(far, 1, far).wait_recv()
    to_sib2 = send(far, 2, sib)
    to_sib2.start()
    norm(far)
    send(far_sib, 2, sib).wait_recv()
    norm(far_sib)

    lab_all = jnp.concatenate([labels_of(s) for s in range(4)], axis=1)
    mask_all = jnp.concatenate([hx[s, pl.ds(SEQ, 1), pl.ds(SEQ, SEQ)] for s in range(4)], axis=1)
    n_tok = 4 * SEQ
    lane = lax.broadcasted_iota(jnp.int32, (1, n_tok), 1)
    up = lax.broadcasted_iota(jnp.int32, (n_tok, n_tok), 0)
    across = lax.broadcasted_iota(jnp.int32, (n_tok, n_tok), 1)
    before = jnp.where((up < across) & (up // BLOCK == across // BLOCK), 1.0, 0.0).astype(jnp.bfloat16)
    rank = dot(jnp.broadcast_to(mask_all, (8, n_tok)).astype(jnp.bfloat16), before, ((1,), (0,)))[0:1, :]
    count_0 = jnp.sum(mask_all[:, :BLOCK], axis=1, keepdims=True)
    count_1 = jnp.sum(mask_all[:, BLOCK:], axis=1, keepdims=True)
    count = count_0 + count_1
    one_block = count <= BLOCK
    base_1 = jnp.where(one_block, BLOCK, 2 * BLOCK) - count_1
    col = jnp.where(lane < BLOCK, rank, rank + base_1)
    col = jnp.where(mask_all > 0.0, col, -1.0).astype(jnp.int32)
    chosen = up == col
    packing = jnp.where(chosen, 1.0, 0.0)
    packing_16 = packing.astype(jnp.bfloat16)
    zc_ref[...] = dot(packing_16, z_all[...], ((1,), (0,))).astype(jnp.bfloat16)
    zt_ref[...] = dot(z_all[...], packing_16, ((0,), (1,))).astype(jnp.bfloat16)

    window = jnp.where(one_block, 0, x * BLOCK)
    mine = jnp.where(x == 0, col[:, :BLOCK], col[:, BLOCK:]) - window
    w_pack = jnp.where(lax.broadcasted_iota(jnp.int32, (BLOCK, BLOCK), 0) == mine, 1.0, 0.0)
    hw_ref[...] = dot(w_pack.astype(jnp.bfloat16), h_chip[...], ((1,), (0,))).astype(jnp.bfloat16)
    wmask_ref[...] = jnp.broadcast_to(jnp.sum(w_pack, axis=1, keepdims=True), (BLOCK, 128))
    own = jnp.where(c == 0, mine[:, :SEQ], mine[:, SEQ:])
    pos_ref[...] = jnp.broadcast_to(own, (8, SEQ))

    def wait_stat(k, carry):
        stat(k, lax.rem(me + k, n_dev)).wait_recv()
        return carry

    lax.fori_loop(1, n_dev, wait_stat, 0)
    lse, goal = [], []
    for group in range(2):
        ids = [t * 4 + 2 * group + k for t in range(n_tp) for k in range(2)]
        parts = [st[d, pl.ds(0, 1), :] for d in ids]
        m = functools.reduce(jnp.maximum, parts)
        lse.append(m + jnp.log(sum(jnp.exp(p - m) for p in parts)))
        goal.append(sum(st[d, pl.ds(1, 1), :] for d in ids))
    lse, goal = jnp.concatenate(lse, axis=1), jnp.concatenate(goal, axis=1)
    loss = jnp.sum(mask_all * (lse - goal), axis=1, keepdims=True) / count

    values = jnp.concatenate([lse, lab_all, jnp.ones((6, n_tok), jnp.float32)], axis=0)
    packed = dot(values, packing, ((1,), (1,)), lax.Precision.HIGHEST)
    used = jnp.sum(jnp.where(packed[2:3, :] > 0.5, 1.0, 0.0), axis=0, keepdims=True)
    stats_ref[pl.ds(0, 1), :] = jnp.where(used > 0.5, packed[0:1, :], 1e30)
    stats_ref[pl.ds(1, 1), :] = jnp.where(used > 0.5, packed[1:2, :], -1.0)
    stats_ref[pl.ds(2, 1), :] = jnp.broadcast_to(1.0 / count, (1, n_tok))
    stats_ref[pl.ds(3, 1), :] = jnp.broadcast_to(count, (1, n_tok))
    stats_ref[pl.ds(4, 1), :] = jnp.broadcast_to(loss, (1, n_tok))
    stats_ref[pl.ds(5, 3), :] = jnp.zeros((3, n_tok), jnp.float32)

    to_sib.wait_send()
    to_far.wait_send()
    to_sib2.wait_send()

    def wait_sent(k, carry):
        stat(k, me).wait_send()
        return carry

    lax.fori_loop(1, n_dev, wait_sent, 0)


def back_kernel(tile, resident, slots, t_0, t_1, *refs):
    if resident:
        embed_ref, zc_ref, zt_ref, stats_ref, out_ref, dz_ref, logit, grad, staged, out_sem = refs
    else:
        embed_ref, zc_ref, zt_ref, stats_ref, _, out_ref, logit, grad, staged, out_sem, held, in_sem = refs
    tp, dp = lax.axis_index('tp'), lax.axis_index('dp')
    chip, c = dp // 2, dp % 2
    rows = out_ref.shape[0]
    vocab_0, row_0 = tp * rows, (c if resident else 1 - c) * (rows // 2)
    count = jnp.max(stats_ref[pl.ds(3, 1), :])
    chunk = tile // 2 if tile % (2 * 16) == 0 else tile
    piece = chunk // 5 if chunk % 80 == 0 else chunk
    width = zc_ref.shape[1]

    def fetch(i):
        slot = lax.rem(i, IN_SLOTS)
        return pltpu.make_async_copy(embed_ref.at[pl.ds(pl.multiple_of(row_0 + i * tile, 16), tile)], held.at[slot], in_sem.at[slot])

    def rows_of(i, r, n):
        if resident:
            return embed_ref[pl.ds(pl.multiple_of(i * tile + r, 16), n), :]
        return held[lax.rem(i, IN_SLOTS), pl.ds(r, n), :]

    def put(i):
        slot = lax.rem(i, slots)
        return pltpu.make_async_copy(staged.at[slot], out_ref.at[pl.ds(pl.multiple_of(row_0 + i * tile, 16), tile)], out_sem.at[slot])

    def run(blocks):
        cols = blocks * BLOCK
        lse = stats_ref[pl.ds(0, 1), pl.ds(0, cols)]
        label = stats_ref[pl.ds(1, 1), pl.ds(0, cols)].astype(jnp.int32) - (vocab_0 + row_0)
        scale = stats_ref[pl.ds(2, 1), pl.ds(0, cols)]
        row_iota = lax.broadcasted_iota(jnp.int32, (piece, cols), 0)

        def product(i, r):
            logit[pl.ds(r, chunk), pl.ds(0, cols)] = dot(rows_of(i, r, chunk), zt_ref[:, pl.ds(0, cols)], ((1,), (0,)))

        if not resident:
            for k in range(IN_SLOTS - 1):
                if t_0 + k < t_1:
                    fetch(t_0 + k).start()
            fetch(t_0).wait()
        else:
            dz_ref[...] = jnp.zeros_like(dz_ref)
        for r in range(0, tile, chunk):
            product(t_0, r)

        def body(i, carry):
            later = jnp.minimum(i + 1, t_1 - 1)
            if not resident:
                @pl.when(i + IN_SLOTS - 1 < t_1)
                def _():
                    fetch(i + IN_SLOTS - 1).start()

                @pl.when(i + 1 < t_1)
                def _():
                    fetch(i + 1).wait()

            @pl.when(i - slots >= t_0)
            def _():
                put(i - slots).wait()

            here = label - i * tile
            for q in range(0, tile, chunk):
                for r in range(q, q + chunk, piece):
                    p = jnp.exp(logit[pl.ds(r, piece), pl.ds(0, cols)] - lse)
                    g = jnp.where(row_iota == here - r, p - 1.0, p) * scale
                    grad[pl.ds(r, piece), pl.ds(0, cols)] = g.astype(jnp.bfloat16)
                product(later, q)
                staged[lax.rem(i, slots), pl.ds(q, chunk), :] = dot(grad[pl.ds(q, chunk), pl.ds(0, cols)], zc_ref[pl.ds(0, cols), :], ((1,), (0,)))
            if resident:
                window = grad[:, pl.ds(0, BLOCK)]
                if blocks > 1:
                    window = jnp.where(chip == 0, window, grad[:, pl.ds(BLOCK, BLOCK)])
                for n in range(0, width, 256):
                    dz_ref[:, pl.ds(n, 256)] += dot(window, rows_of(i, 0, tile)[:, n:n + 256], ((0,), (0,)))
            put(i).start()
            return carry

        lax.fori_loop(t_0, t_1, body, 0)

        def drain(i, carry):
            put(i).wait()
            return carry

        lax.fori_loop(max(t_0, t_1 - slots), t_1, drain, 0)

    @pl.when(count <= BLOCK)
    def _():
        run(1)

    @pl.when(count > BLOCK)
    def _():
        run(2)


def add_kernel(dz_ref, arrived_ref, out_ref):
    lower = out_ref.shape[0]
    at = pl.multiple_of(lax.rem(lax.axis_index('dp'), 2) * lower, 8)
    out_ref[...] = dz_ref[pl.ds(at, lower), :] + arrived_ref[...]


def norm_kernel(hw_ref, wmask_ref, gamma_ref, beta_ref, got_ref, packet_ref):
    n_tp, share, width = got_ref.shape
    dz = functools.reduce(jnp.add, [got_ref[k] for k in range(n_tp)])
    at = pl.multiple_of(lax.rem(lax.axis_index('dp'), 2) * (n_tp * share) + lax.axis_index('tp') * share, 8)
    gamma = gamma_ref[...]
    x_hat, inv_std, _ = layer_norm(hw_ref[pl.ds(at, share), :].astype(jnp.float32), gamma, beta_ref[...])
    scaled = dz * gamma
    d_h = (scaled - jnp.mean(scaled, axis=-1, keepdims=True) - x_hat * jnp.mean(scaled * x_hat, axis=-1, keepdims=True)) * inv_std
    kept = dz * wmask_ref[pl.ds(at, share), pl.ds(0, 1)]
    d_gamma = jnp.sum(kept * x_hat, axis=0, keepdims=True)
    d_beta = jnp.sum(kept, axis=0, keepdims=True)
    row = lax.broadcasted_iota(jnp.int32, (8, width), 0)
    sums = jnp.where(row == 0, d_gamma, jnp.where(row == 1, d_beta, 0.0))
    for k in range(n_tp):
        packet_ref[k, pl.ds(0, share), :] = d_h
        packet_ref[k, pl.ds(share, 8), :] = sums


def order_kernel(packets_ref, win_ref, sums_ref):
    n_tp, share = packets_ref.shape[0], packets_ref.shape[1] - 8
    for k in range(n_tp):
        win_ref[pl.ds(k * share, share), :] = packets_ref[k, pl.ds(0, share), :]
    sums_ref[...] = functools.reduce(jnp.add, [packets_ref[k, pl.ds(share, 8), :] for k in range(n_tp)])


def finish_kernel(pos_ref, stats_ref, win_ref, other_ref, *refs):
    per_dp, (hidden_ref, gamma_ref, beta_ref, loss_ref) = refs[:4], refs[4:]
    dp = lax.axis_index('dp')
    total = jnp.zeros_like(per_dp[0])
    for owner in range(4):
        term = per_dp[0][...]
        for k in range(1, 4):
            term = jnp.where(lax.rem(dp + k, 4) == owner, per_dp[k][...], term)
        total = total + term
    gamma_ref[...] = total[0:1, :]
    beta_ref[...] = total[1:2, :]
    loss_ref[...] = stats_ref[4:5, 0:1]
    lower = win_ref.shape[0]
    slot = pos_ref[0:1, :] - lax.rem(dp, 2) * lower
    slot = jnp.where(slot < 0, slot + 2 * lower, slot)
    slot = jnp.where(pos_ref[0:1, :] < 0, -1, slot)
    up = lax.broadcasted_iota(jnp.int32, (lower, slot.shape[1]), 0)
    out = jnp.zeros(hidden_ref.shape, jnp.float32)
    for part, ref in enumerate((win_ref, other_ref)):
        pick = jnp.where(up + part * lower == slot, 1.0, 0.0).astype(jnp.bfloat16)
        out = out + dot(pick, ref[...].astype(jnp.bfloat16), ((0,), (0,)))
    hidden_ref[...] = out.astype(jnp.bfloat16)


VMEM = pl.BlockSpec(memory_space=pltpu.VMEM)
ANY = pl.BlockSpec(memory_space=pl.ANY)


def solution(mesh):
    n_tp, n_dp = mesh.shape['tp'], mesh.shape['dp']

    def local_step(hidden, ln_gamma, ln_beta, embed, labels, loss_mask):
        tp, dp = lax.axis_index('tp'), lax.axis_index('dp')
        rows, width = embed.shape
        half = rows // 2
        tile = 1120 if half % 1120 == 0 else half // 7
        tiles = half // tile
        x, c = dp // 2, dp % 2
        f32, bf16 = jnp.float32, jnp.bfloat16

        e_half, zc, zt, hw, wmask, stats, pos = pl.pallas_call(
            functools.partial(front_kernel, n_tp, rows, tile),
            out_shape=(pltpu.VMEM((half, width), bf16), jax.ShapeDtypeStruct((4 * SEQ, width), bf16), jax.ShapeDtypeStruct((width, 4 * SEQ), bf16),
                       jax.ShapeDtypeStruct((BLOCK, width), bf16), jax.ShapeDtypeStruct((BLOCK, 128), f32),
                       jax.ShapeDtypeStruct((8, 4 * SEQ), f32), jax.ShapeDtypeStruct((8, SEQ), jnp.int32)),
            in_specs=[ANY] * 6,
            out_specs=[VMEM] * 7,
            scratch_shapes=[
                pltpu.VMEM((SEQ, width), bf16), pltpu.VMEM((1, width), f32), pltpu.VMEM((1, width), f32),
                pltpu.VMEM((1, SEQ), jnp.int32), pltpu.VMEM((1, SEQ), jnp.int32),
                pltpu.VMEM((4, SEQ + 8, width), f32), pltpu.VMEM((4 * SEQ, width), bf16), pltpu.VMEM((BLOCK, width), bf16),
                pltpu.VMEM((tile, BLOCK), f32), pltpu.VMEM((4 * n_tp, 2, BLOCK), f32),
                pltpu.SemaphoreType.DMA((5,)), pltpu.SemaphoreType.DMA((tiles,)), pltpu.SemaphoreType.DMA((3,)), pltpu.SemaphoreType.DMA((3,)),
                pltpu.SemaphoreType.DMA((4 * n_tp,)), pltpu.SemaphoreType.DMA((4 * n_tp,)),
            ],
            compiler_params=pltpu.CompilerParams(collective_id=0, has_side_effects=True, vmem_limit_bytes=12 << 20),
            cost_estimate=pl.CostEstimate(flops=2 * half * BLOCK * width, bytes_accessed=2 * half * width, transcendentals=0),
        )(*[pltpu.with_memory_space_constraint(v, pltpu.HBM) for v in (hidden[0], ln_gamma[None], ln_beta[None], labels, loss_mask, embed)])

        def back(resident, source, t_0, t_1, d_embed=None):
            slots = 2 if resident else 3
            scratch = [pltpu.VMEM((tile, 2 * BLOCK), f32), pltpu.VMEM((tile, 2 * BLOCK), bf16),
                       pltpu.VMEM((slots, tile, width), f32), pltpu.SemaphoreType.DMA((slots,))]
            ops, specs = [source, zc, zt, stats], [VMEM if resident else ANY, VMEM, VMEM, VMEM]
            shapes, outs, alias = [jax.ShapeDtypeStruct((rows, width), f32)], [ANY], {}
            if resident:
                shapes.append(jax.ShapeDtypeStruct((BLOCK, width), f32))
                outs.append(VMEM)
            else:
                ops.append(d_embed)
                specs.append(ANY)
                alias = {4: 0}
                scratch += [pltpu.VMEM((IN_SLOTS, tile, width), bf16), pltpu.SemaphoreType.DMA((IN_SLOTS,))]
            n = t_1 - t_0
            return pl.pallas_call(
                functools.partial(back_kernel, tile, resident, slots, t_0, t_1), out_shape=shapes, in_specs=specs, out_specs=outs,
                scratch_shapes=scratch, input_output_aliases=alias,
                compiler_params=pltpu.CompilerParams(vmem_limit_bytes=(16 if resident else 34) << 20, has_side_effects=True),
                cost_estimate=pl.CostEstimate(flops=6 * n * tile * BLOCK * width, bytes_accessed=6 * n * tile * width, transcendentals=0),
            )(*ops)

        d_embed, dz = back(True, e_half, 0, tiles)

        def small(body, out_shape, *ops):
            return pl.pallas_call(
                body, out_shape=out_shape, in_specs=[VMEM] * len(ops), out_specs=jax.tree.map(lambda _: VMEM, out_shape),
                compiler_params=pltpu.CompilerParams(vmem_limit_bytes=8 << 20),
                cost_estimate=pl.CostEstimate(flops=1 << 20, bytes_accessed=1 << 20, transcendentals=0),
            )(*ops)

        def shape(*dims):
            return jax.ShapeDtypeStruct(dims, f32)

        lower = BLOCK // 2
        share = lower // n_tp
        swap = [(0, 1), (1, 0), (2, 3), (3, 2)]
        arrived = lax.ppermute(lax.dynamic_slice_in_dim(dz, (1 - c) * lower, lower, 0), 'dp', swap)
        dz_half = small(add_kernel, shape(lower, width), dz, arrived)
        got = lax.all_to_all(dz_half.reshape(n_tp, share, width), 'tp', 0, 0)
        d_embed, dz_half = lax.optimization_barrier((d_embed, dz_half))
        (d_embed,) = back(False, embed, 0, tiles // 2, d_embed)
        d_embed, got = lax.optimization_barrier((d_embed, got))

        packets = small(norm_kernel, shape(n_tp, share + 8, width), hw, wmask, ln_gamma[None], ln_beta[None], got)
        packed = lax.all_to_all(packets, 'tp', 0, 0)
        d_embed, packets = lax.optimization_barrier((d_embed, packets))
        (d_embed,) = back(False, embed, tiles // 2, tiles, d_embed)
        d_embed, packed = lax.optimization_barrier((d_embed, packed))

        d_win, sums = small(order_kernel, [shape(lower, width), shape(8, width)], packed)
        other = lax.ppermute(d_win, 'dp', swap)
        per_dp = [sums] + [lax.ppermute(sums, 'dp', [(i, (i - k) % n_dp) for i in range(n_dp)]) for k in range(1, n_dp)]
        d_hidden, d_gamma, d_beta, loss = small(
            finish_kernel, [jax.ShapeDtypeStruct((SEQ, width), bf16), shape(1, width), shape(1, width), shape(1, 1)],
            pos, stats, d_win, other, *per_dp)
        return loss[0, 0], d_hidden[None], d_embed, d_gamma[0], d_beta[0]

    return jax.shard_map(local_step, mesh=mesh, in_specs=(P('dp', None, None), P(None), P(None), P('tp', None), P('dp', None), P('dp', None)), out_specs=(P(), P('dp', None, None), P('tp', None), P(None), P(None)), check_vma=False)
```

```python
import functools

import jax
import jax.numpy as jnp
from jax import lax
from jax.experimental import pallas as pl
from jax.experimental.pallas import tpu as pltpu
from jax.sharding import PartitionSpec as P

MESH = pl.DeviceIdType.MESH
LAYER_EPS = 1e-5
SEQ = 128
BLOCK = 256
IN_SLOTS = 5


def dot(a, b, contract, precision=None):
    return lax.dot_general(a, b, ((contract[0], contract[1]), ((), ())), precision=precision, preferred_element_type=jnp.float32)


def layer_norm(h, gamma, beta):
    centered = h - jnp.mean(h, axis=-1, keepdims=True)
    inv_std = lax.rsqrt(jnp.mean(centered * centered, axis=-1, keepdims=True) + LAYER_EPS)
    x_hat = centered * inv_std
    return x_hat, inv_std, (x_hat * gamma + beta).astype(jnp.bfloat16)


def front_kernel(n_tp, rows, tile, hid_in, gamma_in, beta_in, lab_in, mask_in, embed_ref,
                 half_ref, zc_ref, zt_ref, hw_ref, wmask_ref, stats_ref, pos_ref,
                 hid_ref, gamma_ref, beta_ref, lab_ref, mask_ref, hx, z_all, h_chip, logit, st, in_sem, e_sem, x_send, x_recv, st_send, st_recv):
    tp, dp = lax.axis_index('tp'), lax.axis_index('dp')
    n_dev = n_tp * 4
    me = tp * 4 + dp
    x, c = dp // 2, dp % 2
    sib, far = x * 2 + (1 - c), (1 - x) * 2 + c
    far_sib = (1 - x) * 2 + (1 - c)
    half = rows // 2
    tiles = half // tile
    width = hid_ref.shape[1]
    pairs = ((hid_in, hid_ref), (gamma_in, gamma_ref), (beta_in, beta_ref), (lab_in, lab_ref), (mask_in, mask_ref))
    loads = [pltpu.make_async_copy(a, b, in_sem.at[k]) for k, (a, b) in enumerate(pairs)]
    for load in loads:
        load.start()

    def fetch(i):
        return pltpu.make_async_copy(
            embed_ref.at[pl.ds(pl.multiple_of(c * half + i * tile, 16), tile)],
            half_ref.at[pl.ds(pl.multiple_of(i * tile, 16), tile)], e_sem.at[i])

    def start_fetch(i, carry):
        fetch(i).start()
        return carry

    lax.fori_loop(0, min(IN_SLOTS - 1, tiles), start_fetch, 0)

    barrier = pltpu.get_barrier_semaphore()

    def hello(k, carry):
        peer = lax.rem(me + k, n_dev)
        pl.semaphore_signal(barrier, inc=1, device_id=(peer // 4, lax.rem(peer, 4)), device_id_type=MESH)
        return carry

    lax.fori_loop(1, n_dev, hello, 0)

    for load in loads:
        load.wait()
    lab = jnp.broadcast_to(lab_ref[...].astype(jnp.float32), (8, SEQ))
    msk = jnp.broadcast_to(mask_ref[...].astype(jnp.float32), (8, SEQ))
    hx[dp, pl.ds(SEQ, 8), :] = jnp.concatenate([lab, msk, jnp.zeros((8, width - 2 * SEQ), jnp.float32)], axis=1)

    def widen(r, carry):
        at = pl.ds(pl.multiple_of(r * 32, 32), 32)
        hx[dp, at, :] = hid_ref[at, :].astype(jnp.float32)
        return carry

    lax.fori_loop(0, SEQ // 32, widen, 0)

    def norm(slot):
        def chunk(r, carry):
            at = pl.multiple_of(r * 32, 32)
            h = hx[slot, pl.ds(at, 32), :]
            z_all[pl.ds(pl.multiple_of(slot * SEQ + at, 32), 32), :] = layer_norm(h, gamma_ref[...], beta_ref[...])[2]
            return carry
        lax.fori_loop(0, SEQ // 32, chunk, 0)

    def chip_rows(slot, place):
        def chunk(r, carry):
            at = pl.multiple_of(r * 32, 32)
            h_chip[pl.ds(pl.multiple_of(place * SEQ + at, 32), 32), :] = hx[slot, pl.ds(at, 32), :].astype(jnp.bfloat16)
            return carry
        lax.fori_loop(0, SEQ // 32, chunk, 0)

    norm(dp)
    chip_rows(dp, c)
    pl.semaphore_wait(barrier, n_dev - 1)

    def send(slot, k, to):
        return pltpu.make_async_remote_copy(
            src_ref=hx.at[slot], dst_ref=hx.at[slot], send_sem=x_send.at[k], recv_sem=x_recv.at[k],
            device_id=(tp, to), device_id_type=MESH)

    to_sib, to_far = send(dp, 0, sib), send(dp, 1, far)
    to_far.start()
    to_sib.start()
    send(sib, 0, sib).wait_recv()
    norm(sib)
    chip_rows(sib, 1 - c)

    def labels_of(slot):
        return hx[slot, pl.ds(SEQ, 1), pl.ds(0, SEQ)]

    chip_lab = jnp.concatenate([labels_of(2 * x), labels_of(2 * x + 1)], axis=1).astype(jnp.int32)
    first_row = tp * rows + c * half
    chip_tokens = pl.ds(pl.multiple_of(x * BLOCK, BLOCK), BLOCK)
    piece = tile // 14 if tile % (14 * 8) == 0 else tile

    def product(i):
        logit[...] = dot(half_ref[pl.ds(pl.multiple_of(i * tile, 16), tile), :], z_all[chip_tokens, :], ((1,), (1,)))

    fetch(0).wait()
    product(0)
    row_iota = lax.broadcasted_iota(jnp.int32, (piece, BLOCK), 0)

    def body(i, carry):
        top, total, target = carry
        later = jnp.minimum(i + 1, tiles - 1)

        @pl.when(i + IN_SLOTS - 1 < tiles)
        def _():
            fetch(i + IN_SLOTS - 1).start()

        @pl.when(i + 1 < tiles)
        def _():
            fetch(i + 1).wait()

        new_top = top
        for r in range(0, tile, piece):
            v = logit[pl.ds(r, piece), :].reshape(piece // 8, 8, BLOCK)
            new_top = jnp.maximum(new_top, jnp.max(v, axis=0))
        total = total * jnp.exp(top - new_top)
        lab_here = chip_lab - (first_row + i * tile)
        for r in range(0, tile, piece):
            v = logit[pl.ds(r, piece), :]
            e = jnp.exp(v.reshape(piece // 8, 8, BLOCK) - new_top[None])
            total = total + jnp.sum(e, axis=0)
            hit = jnp.where(row_iota == lab_here - r, v, 0.0)
            target = target + jnp.sum(hit.reshape(piece // 8, 8, BLOCK), axis=0)
        product(later)
        return new_top, total, target

    start = (jnp.full((8, BLOCK), -jnp.inf, jnp.float32), jnp.zeros((8, BLOCK), jnp.float32), jnp.zeros((8, BLOCK), jnp.float32))
    first = jnp.max(logit[...].reshape(tile // 8, 8, BLOCK), axis=0)
    top, total, target = lax.fori_loop(0, tiles, body, (first, start[1], start[2]))

    best = jnp.max(top, axis=0, keepdims=True)
    part = best + jnp.log(jnp.sum(total * jnp.exp(top - best), axis=0, keepdims=True))
    st[me, pl.ds(0, 1), :] = part
    st[me, pl.ds(1, 1), :] = jnp.sum(target, axis=0, keepdims=True)

    def stat(k, owner):
        peer = lax.rem(me + k, n_dev)
        return pltpu.make_async_remote_copy(
            src_ref=st.at[me], dst_ref=st.at[owner], send_sem=st_send.at[k], recv_sem=st_recv.at[owner],
            device_id=(peer // 4, lax.rem(peer, 4)), device_id_type=MESH)

    def send_stat(k, carry):
        stat(k, me).start()
        return carry

    lax.fori_loop(1, n_dev, send_stat, 0)

    send(far, 1, far).wait_recv()
    to_sib2 = send(far, 2, sib)
    to_sib2.start()
    norm(far)
    send(far_sib, 2, sib).wait_recv()
    norm(far_sib)

    lab_all = jnp.concatenate([labels_of(s) for s in range(4)], axis=1)
    mask_all = jnp.concatenate([hx[s, pl.ds(SEQ, 1), pl.ds(SEQ, SEQ)] for s in range(4)], axis=1)
    n_tok = 4 * SEQ
    lane = lax.broadcasted_iota(jnp.int32, (1, n_tok), 1)
    up = lax.broadcasted_iota(jnp.int32, (n_tok, n_tok), 0)
    across = lax.broadcasted_iota(jnp.int32, (n_tok, n_tok), 1)
    before = jnp.where((up < across) & (up // BLOCK == across // BLOCK), 1.0, 0.0).astype(jnp.bfloat16)
    rank = dot(jnp.broadcast_to(mask_all, (8, n_tok)).astype(jnp.bfloat16), before, ((1,), (0,)))[0:1, :]
    count_0 = jnp.sum(mask_all[:, :BLOCK], axis=1, keepdims=True)
    count_1 = jnp.sum(mask_all[:, BLOCK:], axis=1, keepdims=True)
    count = count_0 + count_1
    one_block = count <= BLOCK
    base_1 = jnp.where(one_block, BLOCK, 2 * BLOCK) - count_1
    col = jnp.where(lane < BLOCK, rank, rank + base_1)
    col = jnp.where(mask_all > 0.0, col, -1.0).astype(jnp.int32)
    chosen = up == col
    packing = jnp.where(chosen, 1.0, 0.0)
    packing_16 = packing.astype(jnp.bfloat16)
    zc_ref[...] = dot(packing_16, z_all[...], ((1,), (0,))).astype(jnp.bfloat16)
    zt_ref[...] = dot(z_all[...], packing_16, ((0,), (1,))).astype(jnp.bfloat16)

    window = jnp.where(one_block, 0, x * BLOCK)
    mine = jnp.where(x == 0, col[:, :BLOCK], col[:, BLOCK:]) - window
    w_pack = jnp.where(lax.broadcasted_iota(jnp.int32, (BLOCK, BLOCK), 0) == mine, 1.0, 0.0)
    hw_ref[...] = dot(w_pack.astype(jnp.bfloat16), h_chip[...], ((1,), (0,))).astype(jnp.bfloat16)
    wmask_ref[...] = jnp.broadcast_to(jnp.sum(w_pack, axis=1, keepdims=True), (BLOCK, 128))
    own = jnp.where(c == 0, mine[:, :SEQ], mine[:, SEQ:])
    pos_ref[...] = jnp.broadcast_to(own, (8, SEQ))

    def wait_stat(k, carry):
        stat(k, lax.rem(me + k, n_dev)).wait_recv()
        return carry

    lax.fori_loop(1, n_dev, wait_stat, 0)
    lse, goal = [], []
    for group in range(2):
        ids = [t * 4 + 2 * group + k for t in range(n_tp) for k in range(2)]
        parts = [st[d, pl.ds(0, 1), :] for d in ids]
        m = functools.reduce(jnp.maximum, parts)
        lse.append(m + jnp.log(sum(jnp.exp(p - m) for p in parts)))
        goal.append(sum(st[d, pl.ds(1, 1), :] for d in ids))
    lse, goal = jnp.concatenate(lse, axis=1), jnp.concatenate(goal, axis=1)
    loss = jnp.sum(mask_all * (lse - goal), axis=1, keepdims=True) / count

    values = jnp.concatenate([lse, lab_all, jnp.ones((6, n_tok), jnp.float32)], axis=0)
    packed = dot(values, packing, ((1,), (1,)), lax.Precision.HIGHEST)
    used = jnp.sum(jnp.where(packed[2:3, :] > 0.5, 1.0, 0.0), axis=0, keepdims=True)
    stats_ref[pl.ds(0, 1), :] = jnp.where(used > 0.5, packed[0:1, :], 1e30)
    stats_ref[pl.ds(1, 1), :] = jnp.where(used > 0.5, packed[1:2, :], -1.0)
    stats_ref[pl.ds(2, 1), :] = jnp.broadcast_to(1.0 / count, (1, n_tok))
    stats_ref[pl.ds(3, 1), :] = jnp.broadcast_to(count, (1, n_tok))
    stats_ref[pl.ds(4, 1), :] = jnp.broadcast_to(loss, (1, n_tok))
    stats_ref[pl.ds(5, 3), :] = jnp.zeros((3, n_tok), jnp.float32)

    to_sib.wait_send()
    to_far.wait_send()
    to_sib2.wait_send()

    def wait_sent(k, carry):
        stat(k, me).wait_send()
        return carry

    lax.fori_loop(1, n_dev, wait_sent, 0)


def back_kernel(tile, resident, slots, t_0, t_1, *refs):
    if resident:
        embed_ref, zc_ref, zt_ref, stats_ref, out_ref, dz_ref, logit, grad, staged, out_sem = refs
    else:
        embed_ref, zc_ref, zt_ref, stats_ref, _, out_ref, logit, grad, staged, out_sem, held, in_sem = refs
    tp, dp = lax.axis_index('tp'), lax.axis_index('dp')
    chip, c = dp // 2, dp % 2
    rows = out_ref.shape[0]
    vocab_0, row_0 = tp * rows, (c if resident else 1 - c) * (rows // 2)
    count = jnp.max(stats_ref[pl.ds(3, 1), :])
    chunk = tile // 5 if tile % (5 * 16) == 0 else tile
    piece = chunk // 2 if chunk % 32 == 0 else chunk
    width = zc_ref.shape[1]

    def fetch(i):
        slot = lax.rem(i, IN_SLOTS)
        return pltpu.make_async_copy(embed_ref.at[pl.ds(pl.multiple_of(row_0 + i * tile, 16), tile)], held.at[slot], in_sem.at[slot])

    def rows_of(i, r, n):
        if resident:
            return embed_ref[pl.ds(pl.multiple_of(i * tile + r, 16), n), :]
        return held[lax.rem(i, IN_SLOTS), pl.ds(r, n), :]

    def put(i):
        slot = lax.rem(i, slots)
        return pltpu.make_async_copy(staged.at[slot], out_ref.at[pl.ds(pl.multiple_of(row_0 + i * tile, 16), tile)], out_sem.at[slot])

    def put_piece(i, q):
        slot = lax.rem(i, slots)
        return pltpu.make_async_copy(
            staged.at[slot, pl.ds(q, chunk)], out_ref.at[pl.ds(pl.multiple_of(row_0 + i * tile + q, 16), chunk)], out_sem.at[slot])

    def run(blocks):
        cols = blocks * BLOCK
        by_piece = blocks == 1 and not resident
        lse = stats_ref[pl.ds(0, 1), pl.ds(0, cols)]
        label = stats_ref[pl.ds(1, 1), pl.ds(0, cols)].astype(jnp.int32) - (vocab_0 + row_0)
        scale = stats_ref[pl.ds(2, 1), pl.ds(0, cols)]
        row_iota = lax.broadcasted_iota(jnp.int32, (piece, cols), 0)

        def product(i, r):
            logit[pl.ds(r, chunk), pl.ds(0, cols)] = dot(rows_of(i, r, chunk), zt_ref[:, pl.ds(0, cols)], ((1,), (0,)))

        if not resident:
            for k in range(IN_SLOTS - 1):
                if t_0 + k < t_1:
                    fetch(t_0 + k).start()
            fetch(t_0).wait()
        else:
            dz_ref[...] = jnp.zeros_like(dz_ref)
        for r in range(0, tile, chunk):
            product(t_0, r)

        def body(i, carry):
            later = jnp.minimum(i + 1, t_1 - 1)
            if not resident:
                @pl.when(i + IN_SLOTS - 1 < t_1)
                def _():
                    fetch(i + IN_SLOTS - 1).start()

                @pl.when(i + 1 < t_1)
                def _():
                    fetch(i + 1).wait()

            @pl.when(i - slots >= t_0)
            def _():
                put(i - slots).wait()

            here = label - i * tile
            for q in range(0, tile, chunk):
                for r in range(q, q + chunk, piece):
                    p = jnp.exp(logit[pl.ds(r, piece), pl.ds(0, cols)] - lse)
                    g = jnp.where(row_iota == here - r, p - 1.0, p) * scale
                    grad[pl.ds(r, piece), pl.ds(0, cols)] = g.astype(jnp.bfloat16)
                product(later, q)
                staged[lax.rem(i, slots), pl.ds(q, chunk), :] = dot(grad[pl.ds(q, chunk), pl.ds(0, cols)], zc_ref[pl.ds(0, cols), :], ((1,), (0,)))
                if by_piece:
                    put_piece(i, q).start()
            if resident:
                window = grad[:, pl.ds(0, BLOCK)]
                if blocks > 1:
                    window = jnp.where(chip == 0, window, grad[:, pl.ds(BLOCK, BLOCK)])
                for n in range(0, width, 256):
                    dz_ref[:, pl.ds(n, 256)] += dot(window, rows_of(i, 0, tile)[:, n:n + 256], ((0,), (0,)))
            if not by_piece:
                put(i).start()
            return carry

        lax.fori_loop(t_0, t_1, body, 0)

        def drain(i, carry):
            put(i).wait()
            return carry

        lax.fori_loop(max(t_0, t_1 - slots), t_1, drain, 0)

    @pl.when(count <= BLOCK)
    def _():
        run(1)

    @pl.when(count > BLOCK)
    def _():
        run(2)


def add_kernel(dz_ref, arrived_ref, out_ref):
    lower = out_ref.shape[0]
    at = pl.multiple_of(lax.rem(lax.axis_index('dp'), 2) * lower, 8)
    out_ref[...] = dz_ref[pl.ds(at, lower), :] + arrived_ref[...]


def norm_kernel(hw_ref, wmask_ref, gamma_ref, beta_ref, got_ref, packet_ref):
    n_tp, share, width = got_ref.shape
    dz = functools.reduce(jnp.add, [got_ref[k] for k in range(n_tp)])
    at = pl.multiple_of(lax.rem(lax.axis_index('dp'), 2) * (n_tp * share) + lax.axis_index('tp') * share, 8)
    gamma = gamma_ref[...]
    x_hat, inv_std, _ = layer_norm(hw_ref[pl.ds(at, share), :].astype(jnp.float32), gamma, beta_ref[...])
    scaled = dz * gamma
    d_h = (scaled - jnp.mean(scaled, axis=-1, keepdims=True) - x_hat * jnp.mean(scaled * x_hat, axis=-1, keepdims=True)) * inv_std
    kept = dz * wmask_ref[pl.ds(at, share), pl.ds(0, 1)]
    d_gamma = jnp.sum(kept * x_hat, axis=0, keepdims=True)
    d_beta = jnp.sum(kept, axis=0, keepdims=True)
    row = lax.broadcasted_iota(jnp.int32, (8, width), 0)
    sums = jnp.where(row == 0, d_gamma, jnp.where(row == 1, d_beta, 0.0))
    for k in range(n_tp):
        packet_ref[k, pl.ds(0, share), :] = d_h
        packet_ref[k, pl.ds(share, 8), :] = sums


def order_kernel(packets_ref, win_ref, sums_ref):
    n_tp, share = packets_ref.shape[0], packets_ref.shape[1] - 8
    for k in range(n_tp):
        win_ref[pl.ds(k * share, share), :] = packets_ref[k, pl.ds(0, share), :]
    sums_ref[...] = functools.reduce(jnp.add, [packets_ref[k, pl.ds(share, 8), :] for k in range(n_tp)])


def finish_kernel(pos_ref, stats_ref, win_ref, other_ref, *refs):
    per_dp, (hidden_ref, gamma_ref, beta_ref, loss_ref) = refs[:4], refs[4:]
    dp = lax.axis_index('dp')
    total = jnp.zeros_like(per_dp[0])
    for owner in range(4):
        term = per_dp[0][...]
        for k in range(1, 4):
            term = jnp.where(lax.rem(dp + k, 4) == owner, per_dp[k][...], term)
        total = total + term
    gamma_ref[...] = total[0:1, :]
    beta_ref[...] = total[1:2, :]
    loss_ref[...] = stats_ref[4:5, 0:1]
    lower = win_ref.shape[0]
    slot = pos_ref[0:1, :] - lax.rem(dp, 2) * lower
    slot = jnp.where(slot < 0, slot + 2 * lower, slot)
    slot = jnp.where(pos_ref[0:1, :] < 0, -1, slot)
    up = lax.broadcasted_iota(jnp.int32, (lower, slot.shape[1]), 0)
    out = jnp.zeros(hidden_ref.shape, jnp.float32)
    for part, ref in enumerate((win_ref, other_ref)):
        pick = jnp.where(up + part * lower == slot, 1.0, 0.0).astype(jnp.bfloat16)
        out = out + dot(pick, ref[...].astype(jnp.bfloat16), ((0,), (0,)))
    hidden_ref[...] = out.astype(jnp.bfloat16)


VMEM = pl.BlockSpec(memory_space=pltpu.VMEM)
ANY = pl.BlockSpec(memory_space=pl.ANY)


def solution(mesh):
    n_tp, n_dp = mesh.shape['tp'], mesh.shape['dp']

    def local_step(hidden, ln_gamma, ln_beta, embed, labels, loss_mask):
        tp, dp = lax.axis_index('tp'), lax.axis_index('dp')
        rows, width = embed.shape
        half = rows // 2
        tile = 1120 if half % 1120 == 0 else half // 7
        tiles = half // tile
        x, c = dp // 2, dp % 2
        f32, bf16 = jnp.float32, jnp.bfloat16

        e_half, zc, zt, hw, wmask, stats, pos = pl.pallas_call(
            functools.partial(front_kernel, n_tp, rows, tile),
            out_shape=(pltpu.VMEM((half, width), bf16), jax.ShapeDtypeStruct((4 * SEQ, width), bf16), jax.ShapeDtypeStruct((width, 4 * SEQ), bf16),
                       jax.ShapeDtypeStruct((BLOCK, width), bf16), jax.ShapeDtypeStruct((BLOCK, 128), f32),
                       jax.ShapeDtypeStruct((8, 4 * SEQ), f32), jax.ShapeDtypeStruct((8, SEQ), jnp.int32)),
            in_specs=[ANY] * 6,
            out_specs=[VMEM] * 7,
            scratch_shapes=[
                pltpu.VMEM((SEQ, width), bf16), pltpu.VMEM((1, width), f32), pltpu.VMEM((1, width), f32),
                pltpu.VMEM((1, SEQ), jnp.int32), pltpu.VMEM((1, SEQ), jnp.int32),
                pltpu.VMEM((4, SEQ + 8, width), f32), pltpu.VMEM((4 * SEQ, width), bf16), pltpu.VMEM((BLOCK, width), bf16),
                pltpu.VMEM((tile, BLOCK), f32), pltpu.VMEM((4 * n_tp, 2, BLOCK), f32),
                pltpu.SemaphoreType.DMA((5,)), pltpu.SemaphoreType.DMA((tiles,)), pltpu.SemaphoreType.DMA((3,)), pltpu.SemaphoreType.DMA((3,)),
                pltpu.SemaphoreType.DMA((4 * n_tp,)), pltpu.SemaphoreType.DMA((4 * n_tp,)),
            ],
            compiler_params=pltpu.CompilerParams(collective_id=0, has_side_effects=True, vmem_limit_bytes=12 << 20),
            cost_estimate=pl.CostEstimate(flops=2 * half * BLOCK * width, bytes_accessed=2 * half * width, transcendentals=0),
        )(*[pltpu.with_memory_space_constraint(v, pltpu.HBM) for v in (hidden[0], ln_gamma[None], ln_beta[None], labels, loss_mask, embed)])

        def back(resident, source, t_0, t_1, d_embed=None):
            slots = 3
            scratch = [pltpu.VMEM((tile, 2 * BLOCK), f32), pltpu.VMEM((tile, 2 * BLOCK), bf16),
                       pltpu.VMEM((slots, tile, width), f32), pltpu.SemaphoreType.DMA((slots,))]
            ops, specs = [source, zc, zt, stats], [VMEM if resident else ANY, VMEM, VMEM, VMEM]
            shapes, outs, alias = [jax.ShapeDtypeStruct((rows, width), f32)], [ANY], {}
            if resident:
                shapes.append(jax.ShapeDtypeStruct((BLOCK, width), f32))
                outs.append(VMEM)
            else:
                ops.append(d_embed)
                specs.append(ANY)
                alias = {4: 0}
                scratch += [pltpu.VMEM((IN_SLOTS, tile, width), bf16), pltpu.SemaphoreType.DMA((IN_SLOTS,))]
            n = t_1 - t_0
            return pl.pallas_call(
                functools.partial(back_kernel, tile, resident, slots, t_0, t_1), out_shape=shapes, in_specs=specs, out_specs=outs,
                scratch_shapes=scratch, input_output_aliases=alias,
                compiler_params=pltpu.CompilerParams(vmem_limit_bytes=(19 if resident else 34) << 20, has_side_effects=True),
                cost_estimate=pl.CostEstimate(flops=6 * n * tile * BLOCK * width, bytes_accessed=6 * n * tile * width, transcendentals=0),
            )(*ops)

        d_embed, dz = back(True, e_half, 0, tiles)

        def small(body, out_shape, *ops):
            return pl.pallas_call(
                body, out_shape=out_shape, in_specs=[VMEM] * len(ops), out_specs=jax.tree.map(lambda _: VMEM, out_shape),
                compiler_params=pltpu.CompilerParams(vmem_limit_bytes=8 << 20),
                cost_estimate=pl.CostEstimate(flops=1 << 20, bytes_accessed=1 << 20, transcendentals=0),
            )(*ops)

        def shape(*dims):
            return jax.ShapeDtypeStruct(dims, f32)

        lower = BLOCK // 2
        share = lower // n_tp
        swap = [(0, 1), (1, 0), (2, 3), (3, 2)]
        arrived = lax.ppermute(lax.dynamic_slice_in_dim(dz, (1 - c) * lower, lower, 0), 'dp', swap)
        dz_half = small(add_kernel, shape(lower, width), dz, arrived)
        got = lax.all_to_all(dz_half.reshape(n_tp, share, width), 'tp', 0, 0)
        d_embed, dz_half = lax.optimization_barrier((d_embed, dz_half))
        (d_embed,) = back(False, embed, 0, tiles // 2, d_embed)
        d_embed, got = lax.optimization_barrier((d_embed, got))

        packets = small(norm_kernel, shape(n_tp, share + 8, width), hw, wmask, ln_gamma[None], ln_beta[None], got)
        packed = lax.all_to_all(packets, 'tp', 0, 0)
        d_embed, packets = lax.optimization_barrier((d_embed, packets))
        (d_embed,) = back(False, embed, tiles // 2, tiles, d_embed)
        d_embed, packed = lax.optimization_barrier((d_embed, packed))

        d_win, sums = small(order_kernel, [shape(lower, width), shape(8, width)], packed)
        other = lax.ppermute(d_win, 'dp', swap)
        per_dp = [sums] + [lax.ppermute(sums, 'dp', [(i, (i - k) % n_dp) for i in range(n_dp)]) for k in range(1, n_dp)]
        d_hidden, d_gamma, d_beta, loss = small(
            finish_kernel, [jax.ShapeDtypeStruct((SEQ, width), bf16), shape(1, width), shape(1, width), shape(1, 1)],
            pos, stats, d_win, other, *per_dp)
        return loss[0, 0], d_hidden[None], d_embed, d_gamma[0], d_beta[0]

    return jax.shard_map(local_step, mesh=mesh, in_specs=(P('dp', None, None), P(None), P(None), P('tp', None), P('dp', None), P('dp', None)), out_specs=(P(), P('dp', None, None), P('tp', None), P(None), P(None)), check_vma=False)
```

```python
import functools

import jax
import jax.numpy as jnp
from jax import lax
from jax.experimental import pallas as pl
from jax.experimental.pallas import tpu as pltpu
from jax.sharding import PartitionSpec as P

MESH = pl.DeviceIdType.MESH
LAYER_EPS = 1e-5
SEQ = 128
BLOCK = 256
IN_SLOTS = 5


def dot(a, b, contract, precision=None):
    return lax.dot_general(a, b, ((contract[0], contract[1]), ((), ())), precision=precision, preferred_element_type=jnp.float32)


def layer_norm(h, gamma, beta):
    centered = h - jnp.mean(h, axis=-1, keepdims=True)
    inv_std = lax.rsqrt(jnp.mean(centered * centered, axis=-1, keepdims=True) + LAYER_EPS)
    x_hat = centered * inv_std
    return x_hat, inv_std, (x_hat * gamma + beta).astype(jnp.bfloat16)


def front_kernel(n_tp, rows, tile, hid_in, gamma_in, beta_in, lab_in, mask_in, embed_ref,
                 half_ref, zc_ref, zt_ref, hw_ref, wmask_ref, stats_ref, pos_ref,
                 hid_ref, gamma_ref, beta_ref, lab_ref, mask_ref, hx, z_all, h_chip, logit, st, in_sem, e_sem, x_send, x_recv, st_send, st_recv):
    tp, dp = lax.axis_index('tp'), lax.axis_index('dp')
    n_dev = n_tp * 4
    me = tp * 4 + dp
    x, c = dp // 2, dp % 2
    sib, far = x * 2 + (1 - c), (1 - x) * 2 + c
    far_sib = (1 - x) * 2 + (1 - c)
    half = rows // 2
    tiles = half // tile
    width = hid_ref.shape[1]
    pairs = ((hid_in, hid_ref), (gamma_in, gamma_ref), (beta_in, beta_ref), (lab_in, lab_ref), (mask_in, mask_ref))
    loads = [pltpu.make_async_copy(a, b, in_sem.at[k]) for k, (a, b) in enumerate(pairs)]
    for load in loads:
        load.start()

    def fetch(i):
        return pltpu.make_async_copy(
            embed_ref.at[pl.ds(pl.multiple_of(c * half + i * tile, 16), tile)],
            half_ref.at[pl.ds(pl.multiple_of(i * tile, 16), tile)], e_sem.at[i])

    def start_fetch(i, carry):
        fetch(i).start()
        return carry

    lax.fori_loop(0, min(IN_SLOTS - 1, tiles), start_fetch, 0)

    barrier = pltpu.get_barrier_semaphore()

    def hello(k, carry):
        peer = lax.rem(me + k, n_dev)
        pl.semaphore_signal(barrier, inc=1, device_id=(peer // 4, lax.rem(peer, 4)), device_id_type=MESH)
        return carry

    lax.fori_loop(1, n_dev, hello, 0)

    for load in loads:
        load.wait()
    lab = jnp.broadcast_to(lab_ref[...].astype(jnp.float32), (8, SEQ))
    msk = jnp.broadcast_to(mask_ref[...].astype(jnp.float32), (8, SEQ))
    hx[dp, pl.ds(SEQ, 8), :] = jnp.concatenate([lab, msk, jnp.zeros((8, width - 2 * SEQ), jnp.float32)], axis=1)

    def widen(r, carry):
        at = pl.ds(pl.multiple_of(r * 32, 32), 32)
        hx[dp, at, :] = hid_ref[at, :].astype(jnp.float32)
        return carry

    lax.fori_loop(0, SEQ // 32, widen, 0)

    def norm(slot):
        def chunk(r, carry):
            at = pl.multiple_of(r * 32, 32)
            h = hx[slot, pl.ds(at, 32), :]
            z_all[pl.ds(pl.multiple_of(slot * SEQ + at, 32), 32), :] = layer_norm(h, gamma_ref[...], beta_ref[...])[2]
            return carry
        lax.fori_loop(0, SEQ // 32, chunk, 0)

    def chip_rows(slot, place):
        def chunk(r, carry):
            at = pl.multiple_of(r * 32, 32)
            h_chip[pl.ds(pl.multiple_of(place * SEQ + at, 32), 32), :] = hx[slot, pl.ds(at, 32), :].astype(jnp.bfloat16)
            return carry
        lax.fori_loop(0, SEQ // 32, chunk, 0)

    norm(dp)
    chip_rows(dp, c)
    pl.semaphore_wait(barrier, n_dev - 1)

    def send(slot, k, to):
        return pltpu.make_async_remote_copy(
            src_ref=hx.at[slot], dst_ref=hx.at[slot], send_sem=x_send.at[k], recv_sem=x_recv.at[k],
            device_id=(tp, to), device_id_type=MESH)

    to_sib, to_far = send(dp, 0, sib), send(dp, 1, far)
    to_far.start()
    to_sib.start()
    send(sib, 0, sib).wait_recv()
    norm(sib)
    chip_rows(sib, 1 - c)

    def labels_of(slot):
        return hx[slot, pl.ds(SEQ, 1), pl.ds(0, SEQ)]

    chip_lab = jnp.concatenate([labels_of(2 * x), labels_of(2 * x + 1)], axis=1).astype(jnp.int32)
    first_row = tp * rows + c * half
    chip_tokens = pl.ds(pl.multiple_of(x * BLOCK, BLOCK), BLOCK)
    piece = tile // 14 if tile % (14 * 8) == 0 else tile

    def product(i):
        logit[...] = dot(half_ref[pl.ds(pl.multiple_of(i * tile, 16), tile), :], z_all[chip_tokens, :], ((1,), (1,)))

    fetch(0).wait()
    product(0)
    row_iota = lax.broadcasted_iota(jnp.int32, (piece, BLOCK), 0)

    def absorb(i, carry):
        top, total, target = carry
        later = jnp.minimum(i + 1, tiles - 1)

        @pl.when(i + IN_SLOTS - 1 < tiles)
        def _():
            fetch(i + IN_SLOTS - 1).start()

        @pl.when(i + 1 < tiles)
        def _():
            fetch(i + 1).wait()

        new_top = top
        for r in range(0, tile, piece):
            v = logit[pl.ds(r, piece), :].reshape(piece // 8, 8, BLOCK)
            new_top = jnp.maximum(new_top, jnp.max(v, axis=0))
        total = total * jnp.exp(top - new_top)
        lab_here = chip_lab - (first_row + i * tile)
        for r in range(0, tile, piece):
            v = logit[pl.ds(r, piece), :]
            e = jnp.exp(v.reshape(piece // 8, 8, BLOCK) - new_top[None])
            total = total + jnp.sum(e, axis=0)
            hit = jnp.where(row_iota == lab_here - r, v, 0.0)
            target = target + jnp.sum(hit.reshape(piece // 8, 8, BLOCK), axis=0)
        product(later)
        return new_top, total, target

    start = (jnp.full((8, BLOCK), -jnp.inf, jnp.float32), jnp.zeros((8, BLOCK), jnp.float32), jnp.zeros((8, BLOCK), jnp.float32))
    first = jnp.max(logit[...].reshape(tile // 8, 8, BLOCK), axis=0)
    top, total, target = lax.fori_loop(0, tiles, absorb, (first, start[1], start[2]))

    best = jnp.max(top, axis=0, keepdims=True)
    part = best + jnp.log(jnp.sum(total * jnp.exp(top - best), axis=0, keepdims=True))
    st[me, pl.ds(0, 1), :] = part
    st[me, pl.ds(1, 1), :] = jnp.sum(target, axis=0, keepdims=True)

    def stat(k, owner):
        peer = lax.rem(me + k, n_dev)
        return pltpu.make_async_remote_copy(
            src_ref=st.at[me], dst_ref=st.at[owner], send_sem=st_send.at[k], recv_sem=st_recv.at[owner],
            device_id=(peer // 4, lax.rem(peer, 4)), device_id_type=MESH)

    def send_stat(k, carry):
        stat(k, me).start()
        return carry

    lax.fori_loop(1, n_dev, send_stat, 0)

    send(far, 1, far).wait_recv()
    to_sib2 = send(far, 2, sib)
    to_sib2.start()
    norm(far)
    send(far_sib, 2, sib).wait_recv()
    norm(far_sib)

    lab_all = jnp.concatenate([labels_of(s) for s in range(4)], axis=1)
    mask_all = jnp.concatenate([hx[s, pl.ds(SEQ, 1), pl.ds(SEQ, SEQ)] for s in range(4)], axis=1)
    n_tok = 4 * SEQ
    lane = lax.broadcasted_iota(jnp.int32, (1, n_tok), 1)
    up = lax.broadcasted_iota(jnp.int32, (n_tok, n_tok), 0)
    across = lax.broadcasted_iota(jnp.int32, (n_tok, n_tok), 1)
    before = jnp.where((up < across) & (up // BLOCK == across // BLOCK), 1.0, 0.0).astype(jnp.bfloat16)
    rank = dot(jnp.broadcast_to(mask_all, (8, n_tok)).astype(jnp.bfloat16), before, ((1,), (0,)))[0:1, :]
    count_0 = jnp.sum(mask_all[:, :BLOCK], axis=1, keepdims=True)
    count_1 = jnp.sum(mask_all[:, BLOCK:], axis=1, keepdims=True)
    count = count_0 + count_1
    one_block = count <= BLOCK
    base_1 = jnp.where(one_block, BLOCK, 2 * BLOCK) - count_1
    col = jnp.where(lane < BLOCK, rank, rank + base_1)
    col = jnp.where(mask_all > 0.0, col, -1.0).astype(jnp.int32)
    chosen = up == col
    packing = jnp.where(chosen, 1.0, 0.0)
    packing_16 = packing.astype(jnp.bfloat16)
    zc_ref[...] = dot(packing_16, z_all[...], ((1,), (0,))).astype(jnp.bfloat16)
    zt_ref[...] = dot(z_all[...], packing_16, ((0,), (1,))).astype(jnp.bfloat16)

    window = jnp.where(one_block, 0, x * BLOCK)
    mine = jnp.where(x == 0, col[:, :BLOCK], col[:, BLOCK:]) - window
    w_pack = jnp.where(lax.broadcasted_iota(jnp.int32, (BLOCK, BLOCK), 0) == mine, 1.0, 0.0)
    hw_ref[...] = dot(w_pack.astype(jnp.bfloat16), h_chip[...], ((1,), (0,))).astype(jnp.bfloat16)
    wmask_ref[...] = jnp.broadcast_to(jnp.sum(w_pack, axis=1, keepdims=True), (BLOCK, 128))
    own = jnp.where(c == 0, mine[:, :SEQ], mine[:, SEQ:])
    pos_ref[...] = jnp.broadcast_to(own, (8, SEQ))

    def wait_stat(k, carry):
        stat(k, lax.rem(me + k, n_dev)).wait_recv()
        return carry

    lax.fori_loop(1, n_dev, wait_stat, 0)
    lse, goal = [], []
    for group in range(2):
        ids = [t * 4 + 2 * group + k for t in range(n_tp) for k in range(2)]
        parts = [st[d, pl.ds(0, 1), :] for d in ids]
        m = functools.reduce(jnp.maximum, parts)
        lse.append(m + jnp.log(sum(jnp.exp(p - m) for p in parts)))
        goal.append(sum(st[d, pl.ds(1, 1), :] for d in ids))
    lse, goal = jnp.concatenate(lse, axis=1), jnp.concatenate(goal, axis=1)
    loss = jnp.sum(mask_all * (lse - goal), axis=1, keepdims=True) / count

    values = jnp.concatenate([lse, lab_all, jnp.ones((6, n_tok), jnp.float32)], axis=0)
    packed = dot(values, packing, ((1,), (1,)), lax.Precision.HIGHEST)
    used = jnp.sum(jnp.where(packed[2:3, :] > 0.5, 1.0, 0.0), axis=0, keepdims=True)
    stats_ref[pl.ds(0, 1), :] = jnp.where(used > 0.5, packed[0:1, :], 1e30)
    stats_ref[pl.ds(1, 1), :] = jnp.where(used > 0.5, packed[1:2, :], -1.0)
    stats_ref[pl.ds(2, 1), :] = jnp.broadcast_to(1.0 / count, (1, n_tok))
    stats_ref[pl.ds(3, 1), :] = jnp.broadcast_to(count, (1, n_tok))
    stats_ref[pl.ds(4, 1), :] = jnp.broadcast_to(loss, (1, n_tok))
    stats_ref[pl.ds(5, 3), :] = jnp.zeros((3, n_tok), jnp.float32)

    to_sib.wait_send()
    to_far.wait_send()
    to_sib2.wait_send()

    def wait_sent(k, carry):
        stat(k, me).wait_send()
        return carry

    lax.fori_loop(1, n_dev, wait_sent, 0)


def back_kernel(tile, resident, slots, t_0, t_1, *refs):
    if resident:
        embed_ref, zc_ref, zt_ref, stats_ref, out_ref, dz_ref, logit, grad, staged, out_sem = refs
    else:
        embed_ref, zc_ref, zt_ref, stats_ref, _, out_ref, logit, grad, staged, out_sem, held, in_sem = refs
    tp, dp = lax.axis_index('tp'), lax.axis_index('dp')
    chip, c = dp // 2, dp % 2
    rows = out_ref.shape[0]
    vocab_0, row_0 = tp * rows, (c if resident else 1 - c) * (rows // 2)
    count = jnp.max(stats_ref[pl.ds(3, 1), :])
    chunk = tile // 5 if tile % (5 * 16) == 0 else tile
    piece = chunk // 2 if chunk % 32 == 0 else chunk
    width = zc_ref.shape[1]

    def fetch(i):
        slot = lax.rem(i, IN_SLOTS)
        return pltpu.make_async_copy(embed_ref.at[pl.ds(pl.multiple_of(row_0 + i * tile, 16), tile)], held.at[slot], in_sem.at[slot])

    def rows_of(i, r, n):
        if resident:
            return embed_ref[pl.ds(pl.multiple_of(i * tile + r, 16), n), :]
        return held[lax.rem(i, IN_SLOTS), pl.ds(r, n), :]

    def put(i):
        slot = lax.rem(i, slots)
        return pltpu.make_async_copy(staged.at[slot], out_ref.at[pl.ds(pl.multiple_of(row_0 + i * tile, 16), tile)], out_sem.at[slot])

    def put_piece(i, q):
        slot = lax.rem(i, slots)
        return pltpu.make_async_copy(
            staged.at[slot, pl.ds(q, chunk)], out_ref.at[pl.ds(pl.multiple_of(row_0 + i * tile + q, 16), chunk)], out_sem.at[slot])

    def run(blocks):
        cols = blocks * BLOCK
        unroll = 2 if resident or blocks == 2 else 1
        lse = stats_ref[pl.ds(0, 1), pl.ds(0, cols)]
        label = stats_ref[pl.ds(1, 1), pl.ds(0, cols)].astype(jnp.int32) - (vocab_0 + row_0)
        scale = stats_ref[pl.ds(2, 1), pl.ds(0, cols)]
        row_iota = lax.broadcasted_iota(jnp.int32, (piece, cols), 0)

        def product(i, r):
            logit[pl.ds(r, chunk), pl.ds(0, cols)] = dot(rows_of(i, r, chunk), zt_ref[:, pl.ds(0, cols)], ((1,), (0,)))

        if not resident:
            for k in range(min(IN_SLOTS - 1, t_1 - t_0)):
                fetch(t_0 + k).start()
            fetch(t_0).wait()
        else:
            dz_ref[...] = jnp.zeros_like(dz_ref)
        for r in range(0, tile, chunk):
            product(t_0, r)

        def stage(i, slot, base, last):
            later = jnp.minimum(i + 1, t_1 - 1)
            if not resident and not last:
                @pl.when(i + IN_SLOTS - 1 < t_1)
                def _():
                    fetch(i + IN_SLOTS - 1).start()

                @pl.when(i + 1 < t_1)
                def _():
                    fetch(i + 1).wait()

            @pl.when(i - slots >= t_0)
            def _():
                put(i - slots).wait()

            here = label - i * tile
            for q in range(0, tile, chunk):
                for r in range(q, q + chunk, piece):
                    p = jnp.exp(logit[pl.ds(r, piece), pl.ds(0, cols)] - lse)
                    g = jnp.where(row_iota == here - r, p - 1.0, p) * scale
                    grad[pl.ds(base + r, piece), pl.ds(0, cols)] = g.astype(jnp.bfloat16)
                if not last:
                    product(later, q)
                staged[slot, pl.ds(q, chunk), :] = dot(grad[pl.ds(base + q, chunk), pl.ds(0, cols)], zc_ref[pl.ds(0, cols), :], ((1,), (0,)))
                put_piece(i, q).start()

        def body(p, carry):
            i = t_0 + unroll * p
            for u in range(unroll):
                slot = u if resident else lax.rem(i + u, slots)
                stage(i + u, slot, u * tile if resident else 0, False)
            if resident:
                window = grad[:, pl.ds(0, BLOCK)]
                if blocks > 1:
                    window = jnp.where(chip == 0, window, grad[:, pl.ds(BLOCK, BLOCK)])
                for n in range(0, width, 256):
                    dz_ref[:, pl.ds(n, 256)] += dot(window, rows_of(i, 0, 2 * tile)[:, n:n + 256], ((0,), (0,)))
            return carry

        trips = (t_1 - t_0) // unroll
        lax.fori_loop(0, trips, body, 0)
        if trips * unroll < t_1 - t_0:
            stage(t_1 - 1, (t_1 - 1) % slots, 0, True)

        def drain(i, carry):
            put(i).wait()
            return carry

        lax.fori_loop(max(t_0, t_1 - slots), t_1, drain, 0)

    @pl.when(count <= BLOCK)
    def _():
        run(1)

    @pl.when(count > BLOCK)
    def _():
        run(2)


def add_kernel(dz_ref, arrived_ref, out_ref):
    lower = out_ref.shape[0]
    at = pl.multiple_of(lax.rem(lax.axis_index('dp'), 2) * lower, 8)
    out_ref[...] = dz_ref[pl.ds(at, lower), :] + arrived_ref[...]


def norm_kernel(hw_ref, wmask_ref, gamma_ref, beta_ref, got_ref, packet_ref):
    n_tp, share, width = got_ref.shape
    dz = functools.reduce(jnp.add, [got_ref[k] for k in range(n_tp)])
    at = pl.multiple_of(lax.rem(lax.axis_index('dp'), 2) * (n_tp * share) + lax.axis_index('tp') * share, 8)
    gamma = gamma_ref[...]
    x_hat, inv_std, _ = layer_norm(hw_ref[pl.ds(at, share), :].astype(jnp.float32), gamma, beta_ref[...])
    scaled = dz * gamma
    d_h = (scaled - jnp.mean(scaled, axis=-1, keepdims=True) - x_hat * jnp.mean(scaled * x_hat, axis=-1, keepdims=True)) * inv_std
    kept = dz * wmask_ref[pl.ds(at, share), pl.ds(0, 1)]
    d_gamma = jnp.sum(kept * x_hat, axis=0, keepdims=True)
    d_beta = jnp.sum(kept, axis=0, keepdims=True)
    sums = jnp.concatenate([v[:, n:n + 128] for v in (d_gamma, d_beta) for n in range(0, width, 128)], axis=0)
    for k in range(n_tp):
        packet_ref[k, :, pl.ds(0, width)] = d_h
        packet_ref[k, pl.ds(0, sums.shape[0]), pl.ds(width, 128)] = sums


def order_kernel(packets_ref, win_ref, sums_ref):
    n_tp, share = packets_ref.shape[:2]
    width = win_ref.shape[1]
    for k in range(n_tp):
        win_ref[pl.ds(k * share, share), :] = packets_ref[k, :, pl.ds(0, width)]
    sums_ref[...] = functools.reduce(jnp.add, [packets_ref[k, pl.ds(0, width // 64), pl.ds(width, 128)] for k in range(n_tp)])


def finish_kernel(pos_ref, stats_ref, win_ref, other_ref, *refs):
    per_dp, (hidden_ref, gamma_ref, beta_ref, loss_ref) = refs[:4], refs[4:]
    dp = lax.axis_index('dp')
    total = jnp.zeros_like(per_dp[0])
    for owner in range(4):
        term = per_dp[0][...]
        for k in range(1, 4):
            term = jnp.where(lax.rem(dp + k, 4) == owner, per_dp[k][...], term)
        total = total + term
    lines = total.shape[0] // 2
    gamma_ref[...] = jnp.concatenate([total[n:n + 1, :] for n in range(lines)], axis=1)
    beta_ref[...] = jnp.concatenate([total[n:n + 1, :] for n in range(lines, 2 * lines)], axis=1)
    loss_ref[...] = stats_ref[4:5, 0:1]
    lower = win_ref.shape[0]
    slot = pos_ref[0:1, :] - lax.rem(dp, 2) * lower
    slot = jnp.where(slot < 0, slot + 2 * lower, slot)
    slot = jnp.where(pos_ref[0:1, :] < 0, -1, slot)
    up = lax.broadcasted_iota(jnp.int32, (lower, slot.shape[1]), 0)
    out = jnp.zeros(hidden_ref.shape, jnp.float32)
    for part, ref in enumerate((win_ref, other_ref)):
        pick = jnp.where(up + part * lower == slot, 1.0, 0.0).astype(jnp.bfloat16)
        out = out + dot(pick, ref[...].astype(jnp.bfloat16), ((0,), (0,)))
    hidden_ref[...] = out.astype(jnp.bfloat16)


VMEM = pl.BlockSpec(memory_space=pltpu.VMEM)
ANY = pl.BlockSpec(memory_space=pl.ANY)


def solution(mesh):
    n_tp, n_dp = mesh.shape['tp'], mesh.shape['dp']

    def local_step(hidden, ln_gamma, ln_beta, embed, labels, loss_mask):
        tp, dp = lax.axis_index('tp'), lax.axis_index('dp')
        rows, width = embed.shape
        half = rows // 2
        tile = 1120 if half % 1120 == 0 and half > 1120 else half // 14
        tiles = half // tile
        x, c = dp // 2, dp % 2
        f32, bf16 = jnp.float32, jnp.bfloat16

        e_half, zc, zt, hw, wmask, stats, pos = pl.pallas_call(
            functools.partial(front_kernel, n_tp, rows, tile),
            out_shape=(pltpu.VMEM((half, width), bf16), jax.ShapeDtypeStruct((4 * SEQ, width), bf16), jax.ShapeDtypeStruct((width, 4 * SEQ), bf16),
                       jax.ShapeDtypeStruct((BLOCK, width), bf16), jax.ShapeDtypeStruct((BLOCK, 128), f32),
                       jax.ShapeDtypeStruct((8, 4 * SEQ), f32), jax.ShapeDtypeStruct((8, SEQ), jnp.int32)),
            in_specs=[ANY] * 6,
            out_specs=[VMEM] * 7,
            scratch_shapes=[
                pltpu.VMEM((SEQ, width), bf16), pltpu.VMEM((1, width), f32), pltpu.VMEM((1, width), f32),
                pltpu.VMEM((1, SEQ), jnp.int32), pltpu.VMEM((1, SEQ), jnp.int32),
                pltpu.VMEM((4, SEQ + 8, width), f32), pltpu.VMEM((4 * SEQ, width), bf16), pltpu.VMEM((BLOCK, width), bf16),
                pltpu.VMEM((tile, BLOCK), f32), pltpu.VMEM((4 * n_tp, 2, BLOCK), f32),
                pltpu.SemaphoreType.DMA((5,)), pltpu.SemaphoreType.DMA((tiles,)), pltpu.SemaphoreType.DMA((3,)), pltpu.SemaphoreType.DMA((3,)),
                pltpu.SemaphoreType.DMA((4 * n_tp,)), pltpu.SemaphoreType.DMA((4 * n_tp,)),
            ],
            compiler_params=pltpu.CompilerParams(collective_id=0, has_side_effects=True, vmem_limit_bytes=12 << 20),
            cost_estimate=pl.CostEstimate(flops=2 * half * BLOCK * width, bytes_accessed=2 * half * width, transcendentals=0),
        )(*[pltpu.with_memory_space_constraint(v, pltpu.HBM) for v in (hidden[0], ln_gamma[None], ln_beta[None], labels, loss_mask, embed)])

        def back(resident, source, t_0, t_1, d_embed=None):
            slots = 2 if resident else 3
            scratch = [pltpu.VMEM((tile, 2 * BLOCK), f32), pltpu.VMEM((2 * tile if resident else tile, 2 * BLOCK), bf16),
                       pltpu.VMEM((slots, tile, width), f32), pltpu.SemaphoreType.DMA((slots,))]
            ops, specs = [source, zc, zt, stats], [VMEM if resident else ANY, VMEM, VMEM, VMEM]
            shapes, outs, alias = [jax.ShapeDtypeStruct((rows, width), f32)], [ANY], {}
            if resident:
                shapes.append(jax.ShapeDtypeStruct((BLOCK, width), f32))
                outs.append(VMEM)
            else:
                ops.append(d_embed)
                specs.append(ANY)
                alias = {4: 0}
                scratch += [pltpu.VMEM((IN_SLOTS, tile, width), bf16), pltpu.SemaphoreType.DMA((IN_SLOTS,))]
            n = t_1 - t_0
            return pl.pallas_call(
                functools.partial(back_kernel, tile, resident, slots, t_0, t_1), out_shape=shapes, in_specs=specs, out_specs=outs,
                scratch_shapes=scratch, input_output_aliases=alias,
                compiler_params=pltpu.CompilerParams(vmem_limit_bytes=(19 if resident else 34) << 20, has_side_effects=True),
                cost_estimate=pl.CostEstimate(flops=6 * n * tile * BLOCK * width, bytes_accessed=6 * n * tile * width, transcendentals=0),
            )(*ops)

        d_embed, dz = back(True, e_half, 0, tiles)

        def small(body, out_shape, *ops):
            return pl.pallas_call(
                body, out_shape=out_shape, in_specs=[VMEM] * len(ops), out_specs=jax.tree.map(lambda _: VMEM, out_shape),
                compiler_params=pltpu.CompilerParams(vmem_limit_bytes=8 << 20),
                cost_estimate=pl.CostEstimate(flops=1 << 20, bytes_accessed=1 << 20, transcendentals=0),
            )(*ops)

        def shape(*dims):
            return jax.ShapeDtypeStruct(dims, f32)

        lower = BLOCK // 2
        share = lower // n_tp
        swap = [(0, 1), (1, 0), (2, 3), (3, 2)]
        arrived = lax.ppermute(lax.dynamic_slice_in_dim(dz, (1 - c) * lower, lower, 0), 'dp', swap)
        dz_half = small(add_kernel, shape(lower, width), dz, arrived)
        got = lax.all_to_all(dz_half.reshape(n_tp, share, width), 'tp', 0, 0)
        d_embed, dz_half = lax.optimization_barrier((d_embed, dz_half))
        (d_embed,) = back(False, embed, 0, tiles // 2, d_embed)
        d_embed, got = lax.optimization_barrier((d_embed, got))

        packets = small(norm_kernel, shape(n_tp, share, width + 128), hw, wmask, ln_gamma[None], ln_beta[None], got)
        packed = lax.all_to_all(packets, 'tp', 0, 0)
        d_embed, packets = lax.optimization_barrier((d_embed, packets))
        (d_embed,) = back(False, embed, tiles // 2, tiles, d_embed)
        d_embed, packed = lax.optimization_barrier((d_embed, packed))

        d_win, sums = small(order_kernel, [shape(lower, width), shape(width // 64, 128)], packed)
        other = lax.ppermute(d_win, 'dp', swap)
        per_dp = [sums] + [lax.ppermute(sums, 'dp', [(i, (i - k) % n_dp) for i in range(n_dp)]) for k in range(1, n_dp)]
        d_hidden, d_gamma, d_beta, loss = small(
            finish_kernel, [jax.ShapeDtypeStruct((SEQ, width), bf16), shape(1, width), shape(1, width), shape(1, 1)],
            pos, stats, d_win, other, *per_dp)
        return loss[0, 0], d_hidden[None], d_embed, d_gamma[0], d_beta[0]

    return jax.shard_map(local_step, mesh=mesh, in_specs=(P('dp', None, None), P(None), P(None), P('tp', None), P('dp', None), P('dp', None)), out_specs=(P(), P('dp', None, None), P('tp', None), P(None), P(None)), check_vma=False)
```

```python
import functools

import jax
import jax.numpy as jnp
from jax import lax
from jax.experimental import pallas as pl
from jax.experimental.pallas import tpu as pltpu
from jax.sharding import PartitionSpec as P

MESH = pl.DeviceIdType.MESH
LAYER_EPS = 1e-5
SEQ = 128
BLOCK = 256
IN_SLOTS = 5


def dot(a, b, contract, precision=None):
    return lax.dot_general(a, b, ((contract[0], contract[1]), ((), ())), precision=precision, preferred_element_type=jnp.float32)


def layer_norm(h, gamma, beta):
    centered = h - jnp.mean(h, axis=-1, keepdims=True)
    inv_std = lax.rsqrt(jnp.mean(centered * centered, axis=-1, keepdims=True) + LAYER_EPS)
    x_hat = centered * inv_std
    return x_hat, inv_std, (x_hat * gamma + beta).astype(jnp.bfloat16)


def front_kernel(n_tp, rows, tile, hid_in, gamma_in, beta_in, lab_in, mask_in, embed_ref,
                 half_ref, zc_ref, zt_ref, hw_ref, wmask_ref, stats_ref, pos_ref,
                 hid_ref, gamma_ref, beta_ref, lab_ref, mask_ref, hx, z_all, h_chip, logit, st, in_sem, e_sem, x_send, x_recv, st_send, st_recv):
    tp, dp = lax.axis_index('tp'), lax.axis_index('dp')
    n_dev = n_tp * 4
    me = tp * 4 + dp
    x, c = dp // 2, dp % 2
    sib, far = x * 2 + (1 - c), (1 - x) * 2 + c
    far_sib = (1 - x) * 2 + (1 - c)
    half = rows // 2
    tiles = half // tile
    width = hid_ref.shape[1]
    pairs = ((hid_in, hid_ref), (gamma_in, gamma_ref), (beta_in, beta_ref), (lab_in, lab_ref), (mask_in, mask_ref))
    loads = [pltpu.make_async_copy(a, b, in_sem.at[k]) for k, (a, b) in enumerate(pairs)]
    for load in loads:
        load.start()

    def fetch(i):
        return pltpu.make_async_copy(
            embed_ref.at[pl.ds(pl.multiple_of(c * half + i * tile, 16), tile)],
            half_ref.at[pl.ds(pl.multiple_of(i * tile, 16), tile)], e_sem.at[i])

    def start_fetch(i, carry):
        fetch(i).start()
        return carry

    lax.fori_loop(0, min(IN_SLOTS - 1, tiles), start_fetch, 0)

    barrier = pltpu.get_barrier_semaphore()

    peers = [(dt, dd) for dt in reversed(range(n_tp)) for dd in range(4) if dt or dd]

    def peer(dt, dd):
        return lax.rem(tp + dt, n_tp), lax.rem(dp + dd, 4)

    for dt, dd in peers:
        pl.semaphore_signal(barrier, inc=1, device_id=peer(dt, dd), device_id_type=MESH)

    for load in loads:
        load.wait()
    lab = jnp.broadcast_to(lab_ref[...].astype(jnp.float32), (8, SEQ))
    msk = jnp.broadcast_to(mask_ref[...].astype(jnp.float32), (8, SEQ))
    hx[dp, pl.ds(SEQ, 8), :] = jnp.concatenate([lab, msk, jnp.zeros((8, width - 2 * SEQ), jnp.float32)], axis=1)

    def widen(r, carry):
        at = pl.ds(pl.multiple_of(r * 32, 32), 32)
        hx[dp, at, :] = hid_ref[at, :].astype(jnp.float32)
        return carry

    lax.fori_loop(0, SEQ // 32, widen, 0)

    def norm(slot):
        def chunk(r, carry):
            at = pl.multiple_of(r * 32, 32)
            h = hx[slot, pl.ds(at, 32), :]
            z_all[pl.ds(pl.multiple_of(slot * SEQ + at, 32), 32), :] = layer_norm(h, gamma_ref[...], beta_ref[...])[2]
            return carry
        lax.fori_loop(0, SEQ // 32, chunk, 0)

    def chip_rows(slot, place):
        def chunk(r, carry):
            at = pl.multiple_of(r * 32, 32)
            h_chip[pl.ds(pl.multiple_of(place * SEQ + at, 32), 32), :] = hx[slot, pl.ds(at, 32), :].astype(jnp.bfloat16)
            return carry
        lax.fori_loop(0, SEQ // 32, chunk, 0)

    pl.semaphore_wait(barrier, n_dev - 1)

    def send(slot, k, to):
        return pltpu.make_async_remote_copy(
            src_ref=hx.at[slot], dst_ref=hx.at[slot], send_sem=x_send.at[k], recv_sem=x_recv.at[k],
            device_id=(tp, to), device_id_type=MESH)

    to_sib, to_far = send(dp, 0, sib), send(dp, 1, far)
    to_sib.start()
    to_far.start()
    norm(dp)
    chip_rows(dp, c)
    send(sib, 0, sib).wait_recv()
    norm(sib)
    chip_rows(sib, 1 - c)

    def labels_of(slot):
        return hx[slot, pl.ds(SEQ, 1), pl.ds(0, SEQ)]

    chip_lab = jnp.concatenate([labels_of(2 * x), labels_of(2 * x + 1)], axis=1).astype(jnp.int32)
    first_row = tp * rows + c * half
    chip_tokens = pl.ds(pl.multiple_of(x * BLOCK, BLOCK), BLOCK)
    piece = tile // 14 if tile % (14 * 8) == 0 else tile

    def product(i):
        logit[...] = dot(half_ref[pl.ds(pl.multiple_of(i * tile, 16), tile), :], z_all[chip_tokens, :], ((1,), (1,)))

    fetch(0).wait()
    product(0)
    row_iota = lax.broadcasted_iota(jnp.int32, (piece, BLOCK), 0)

    def absorb(i, carry, last=False):
        top, total, target = carry

        if not last:
            @pl.when(i + IN_SLOTS - 1 < tiles)
            def _():
                fetch(i + IN_SLOTS - 1).start()

            fetch(i + 1).wait()

        new_top = top
        for r in range(0, tile, piece):
            v = logit[pl.ds(r, piece), :].reshape(piece // 8, 8, BLOCK)
            new_top = jnp.maximum(new_top, jnp.max(v, axis=0))
        total = total * jnp.exp(top - new_top)
        lab_here = chip_lab - (first_row + i * tile)
        for r in range(0, tile, piece):
            v = logit[pl.ds(r, piece), :]
            e = jnp.exp(v.reshape(piece // 8, 8, BLOCK) - new_top[None])
            total = total + jnp.sum(e, axis=0)
            hit = jnp.where(row_iota == lab_here - r, v, 0.0)
            target = target + jnp.sum(hit.reshape(piece // 8, 8, BLOCK), axis=0)
        if not last:
            product(i + 1)
        return new_top, total, target

    zero = jnp.zeros((8, BLOCK), jnp.float32)
    carry = lax.fori_loop(0, tiles - 1, absorb, (jnp.full((8, BLOCK), -jnp.inf, jnp.float32), zero, zero))
    top, total, target = absorb(tiles - 1, carry, last=True)

    best = jnp.max(top, axis=0, keepdims=True)
    part = best + jnp.log(jnp.sum(total * jnp.exp(top - best), axis=0, keepdims=True))
    st[me, pl.ds(0, 1), :] = part
    st[me, pl.ds(1, 1), :] = jnp.sum(target, axis=0, keepdims=True)

    def stat(dt, dd, incoming):
        to = peer(dt, dd)
        owner = to[0] * 4 + to[1] if incoming else me
        return pltpu.make_async_remote_copy(
            src_ref=st.at[me], dst_ref=st.at[owner], send_sem=st_send.at[dt * 4 + dd], recv_sem=st_recv.at[owner],
            device_id=to, device_id_type=MESH)

    for dt, dd in peers:
        stat(dt, dd, False).start()

    send(far, 1, far).wait_recv()
    to_sib2 = send(far, 2, sib)
    to_sib2.start()
    norm(far)
    send(far_sib, 2, sib).wait_recv()
    norm(far_sib)

    lab_all = jnp.concatenate([labels_of(s) for s in range(4)], axis=1)
    mask_all = jnp.concatenate([hx[s, pl.ds(SEQ, 1), pl.ds(SEQ, SEQ)] for s in range(4)], axis=1)
    n_tok = 4 * SEQ
    lane = lax.broadcasted_iota(jnp.int32, (1, n_tok), 1)
    up = lax.broadcasted_iota(jnp.int32, (n_tok, n_tok), 0)
    across = lax.broadcasted_iota(jnp.int32, (n_tok, n_tok), 1)
    before = jnp.where((up < across) & (up // BLOCK == across // BLOCK), 1.0, 0.0).astype(jnp.bfloat16)
    rank = dot(jnp.broadcast_to(mask_all, (8, n_tok)).astype(jnp.bfloat16), before, ((1,), (0,)))[0:1, :]
    count_0 = jnp.sum(mask_all[:, :BLOCK], axis=1, keepdims=True)
    count_1 = jnp.sum(mask_all[:, BLOCK:], axis=1, keepdims=True)
    count = count_0 + count_1
    one_block = count <= BLOCK
    base_1 = jnp.where(one_block, BLOCK, 2 * BLOCK) - count_1
    col = jnp.where(lane < BLOCK, rank, rank + base_1)
    col = jnp.where(mask_all > 0.0, col, -1.0).astype(jnp.int32)
    chosen = up == col
    packing = jnp.where(chosen, 1.0, 0.0)
    packing_16 = packing.astype(jnp.bfloat16)
    zc_ref[...] = dot(packing_16, z_all[...], ((1,), (0,))).astype(jnp.bfloat16)
    zt_ref[...] = dot(z_all[...], packing_16, ((0,), (1,))).astype(jnp.bfloat16)

    window = jnp.where(one_block, 0, x * BLOCK)
    mine = jnp.where(x == 0, col[:, :BLOCK], col[:, BLOCK:]) - window
    w_pack = jnp.where(lax.broadcasted_iota(jnp.int32, (BLOCK, BLOCK), 0) == mine, 1.0, 0.0)
    hw_ref[...] = dot(w_pack.astype(jnp.bfloat16), h_chip[...], ((1,), (0,))).astype(jnp.bfloat16)
    wmask_ref[...] = jnp.broadcast_to(jnp.sum(w_pack, axis=1, keepdims=True), (BLOCK, 128))
    own = jnp.where(c == 0, mine[:, :SEQ], mine[:, SEQ:])
    pos_ref[...] = jnp.broadcast_to(own, (8, SEQ))

    to_sib.wait_send()
    to_far.wait_send()
    to_sib2.wait_send()
    for dt, dd in peers:
        stat(dt, dd, False).wait_send()
    for dt, dd in peers:
        stat(dt, dd, True).wait_recv()
    lse, goal = [], []
    for group in range(2):
        ids = [t * 4 + 2 * group + k for t in range(n_tp) for k in range(2)]
        parts = [st[d, pl.ds(0, 1), :] for d in ids]
        m = functools.reduce(jnp.maximum, parts)
        lse.append(m + jnp.log(sum(jnp.exp(p - m) for p in parts)))
        goal.append(sum(st[d, pl.ds(1, 1), :] for d in ids))
    lse, goal = jnp.concatenate(lse, axis=1), jnp.concatenate(goal, axis=1)
    loss = jnp.sum(mask_all * (lse - goal), axis=1, keepdims=True) / count

    values = jnp.concatenate([lse, lab_all, jnp.ones((6, n_tok), jnp.float32)], axis=0)
    packed = dot(values, packing, ((1,), (1,)), lax.Precision.HIGHEST)
    used = jnp.sum(jnp.where(packed[2:3, :] > 0.5, 1.0, 0.0), axis=0, keepdims=True)
    stats_ref[pl.ds(0, 1), :] = jnp.where(used > 0.5, packed[0:1, :], 1e30)
    stats_ref[pl.ds(1, 1), :] = jnp.where(used > 0.5, packed[1:2, :], -1.0)
    stats_ref[pl.ds(2, 1), :] = jnp.broadcast_to(1.0 / count, (1, n_tok))
    stats_ref[pl.ds(3, 1), :] = jnp.broadcast_to(count, (1, n_tok))
    stats_ref[pl.ds(4, 1), :] = jnp.broadcast_to(loss, (1, n_tok))
    stats_ref[pl.ds(5, 3), :] = jnp.zeros((3, n_tok), jnp.float32)


def back_kernel(tile, resident, slots, spans, *refs):
    if resident:
        embed_ref, zc_ref, zt_ref, stats_ref, out_ref, dz_ref, logit, grad, staged, out_sem = refs
    else:
        embed_ref, zc_ref, zt_ref, stats_ref, _, out_ref, logit, grad, staged, out_sem, held, in_sem, first_sem = refs
    tp, dp = lax.axis_index('tp'), lax.axis_index('dp')
    chip, c = dp // 2, dp % 2
    rows = out_ref.shape[0]
    vocab_0, row_0 = tp * rows, (c if resident else 1 - c) * (rows // 2)
    count = jnp.max(stats_ref[pl.ds(3, 1), :])
    chunk = tile // 5 if tile % (5 * 16) == 0 else tile
    piece = chunk // 2 if chunk % 32 == 0 else chunk
    width = zc_ref.shape[1]

    def fetch(i):
        slot = lax.rem(i, IN_SLOTS)
        return pltpu.make_async_copy(embed_ref.at[pl.ds(pl.multiple_of(row_0 + i * tile, 16), tile)], held.at[slot], in_sem.at[slot])

    def fetch_piece(t_0, r):
        return pltpu.make_async_copy(
            embed_ref.at[pl.ds(pl.multiple_of(row_0 + t_0 * tile + r, 16), chunk)], held.at[t_0 % IN_SLOTS, pl.ds(r, chunk)], first_sem.at[r // chunk])

    def rows_of(i, r, n):
        if resident:
            return embed_ref[pl.ds(pl.multiple_of(i * tile + r, 16), n), :]
        return held[lax.rem(i, IN_SLOTS), pl.ds(r, n), :]

    def put(i):
        slot = lax.rem(i, slots)
        return pltpu.make_async_copy(staged.at[slot], out_ref.at[pl.ds(pl.multiple_of(row_0 + i * tile, 16), tile)], out_sem.at[slot])

    def put_piece(i, q):
        slot = lax.rem(i, slots)
        return pltpu.make_async_copy(
            staged.at[slot, pl.ds(q, chunk)], out_ref.at[pl.ds(pl.multiple_of(row_0 + i * tile + q, 16), chunk)], out_sem.at[slot])

    def run(blocks):
        cols = blocks * BLOCK
        t_0, t_1 = spans[blocks - 1]
        unroll = 2 if resident or blocks == 2 else 1
        lse = stats_ref[pl.ds(0, 1), pl.ds(0, cols)]
        label = stats_ref[pl.ds(1, 1), pl.ds(0, cols)].astype(jnp.int32) - (vocab_0 + row_0)
        scale = stats_ref[pl.ds(2, 1), pl.ds(0, cols)]
        row_iota = lax.broadcasted_iota(jnp.int32, (piece, cols), 0)

        def product(i, r):
            logit[pl.ds(r, chunk), pl.ds(0, cols)] = dot(rows_of(i, r, chunk), zt_ref[:, pl.ds(0, cols)], ((1,), (0,)))

        if not resident:
            for r in range(0, tile, chunk):
                fetch_piece(t_0, r).start()
            for k in range(1, min(IN_SLOTS - 1, t_1 - t_0)):
                fetch(t_0 + k).start()
        else:
            dz_ref[...] = jnp.zeros_like(dz_ref)
        for r in range(0, tile, chunk):
            if not resident:
                fetch_piece(t_0, r).wait()
            product(t_0, r)

        def stage(i, slot, base, last):
            later = jnp.minimum(i + 1, t_1 - 1)
            if not resident and not last:
                @pl.when(i + IN_SLOTS - 1 < t_1)
                def _():
                    fetch(i + IN_SLOTS - 1).start()

                @pl.when(i + 1 < t_1)
                def _():
                    fetch(i + 1).wait()

            @pl.when(i - slots >= t_0)
            def _():
                put(i - slots).wait()

            here = label - i * tile
            for q in range(0, tile, chunk):
                for r in range(q, q + chunk, piece):
                    p = jnp.exp(logit[pl.ds(r, piece), pl.ds(0, cols)] - lse)
                    g = jnp.where(row_iota == here - r, p - 1.0, p) * scale
                    grad[pl.ds(base + r, piece), pl.ds(0, cols)] = g.astype(jnp.bfloat16)
                if not last:
                    product(later, q)
                staged[slot, pl.ds(q, chunk), :] = dot(grad[pl.ds(base + q, chunk), pl.ds(0, cols)], zc_ref[pl.ds(0, cols), :], ((1,), (0,)))
                put_piece(i, q).start()

        def body(p, carry):
            i = t_0 + unroll * p
            for u in range(unroll):
                slot = u if resident else lax.rem(i + u, slots)
                stage(i + u, slot, u * tile if resident else 0, False)
            if resident:
                window = grad[:, pl.ds(0, BLOCK)]
                if blocks > 1:
                    window = jnp.where(chip == 0, window, grad[:, pl.ds(BLOCK, BLOCK)])
                for n in range(0, width, 256):
                    dz_ref[:, pl.ds(n, 256)] += dot(window, rows_of(i, 0, 2 * tile)[:, n:n + 256], ((0,), (0,)))
            return carry

        trips = (t_1 - t_0) // unroll
        lax.fori_loop(0, trips, body, 0)
        if trips * unroll < t_1 - t_0:
            stage(t_1 - 1, (t_1 - 1) % slots, 0, True)

        def drain(i, carry):
            put(i).wait()
            return carry

        lax.fori_loop(max(t_0, t_1 - slots), t_1, drain, 0)

    @pl.when(count <= BLOCK)
    def _():
        run(1)

    @pl.when(count > BLOCK)
    def _():
        run(2)


def add_kernel(dz_ref, arrived_ref, out_ref):
    lower = out_ref.shape[0]
    at = pl.multiple_of(lax.rem(lax.axis_index('dp'), 2) * lower, 8)
    out_ref[...] = dz_ref[pl.ds(at, lower), :] + arrived_ref[...]


def norm_kernel(hw_ref, wmask_ref, gamma_ref, beta_ref, got_ref, packet_ref):
    n_tp, share, width = got_ref.shape
    dz = functools.reduce(jnp.add, [got_ref[k] for k in range(n_tp)])
    at = pl.multiple_of(lax.rem(lax.axis_index('dp'), 2) * (n_tp * share) + lax.axis_index('tp') * share, 8)
    gamma = gamma_ref[...]
    x_hat, inv_std, _ = layer_norm(hw_ref[pl.ds(at, share), :].astype(jnp.float32), gamma, beta_ref[...])
    scaled = dz * gamma
    d_h = (scaled - jnp.mean(scaled, axis=-1, keepdims=True) - x_hat * jnp.mean(scaled * x_hat, axis=-1, keepdims=True)) * inv_std
    kept = dz * wmask_ref[pl.ds(at, share), pl.ds(0, 1)]
    d_gamma = jnp.sum(kept * x_hat, axis=0, keepdims=True)
    d_beta = jnp.sum(kept, axis=0, keepdims=True)
    sums = jnp.concatenate([v[:, n:n + 128] for v in (d_gamma, d_beta) for n in range(0, width, 128)], axis=0)
    for k in range(n_tp):
        packet_ref[k, :, pl.ds(0, width)] = d_h
        packet_ref[k, pl.ds(0, sums.shape[0]), pl.ds(width, 128)] = sums


def order_kernel(packets_ref, win_ref, sums_ref):
    n_tp, share = packets_ref.shape[:2]
    width = win_ref.shape[1]
    for k in range(n_tp):
        win_ref[pl.ds(k * share, share), :] = packets_ref[k, :, pl.ds(0, width)]
    sums = functools.reduce(jnp.add, [packets_ref[k, pl.ds(0, width // 64), pl.ds(width, 128)] for k in range(n_tp)])
    for k in range(sums_ref.shape[0]):
        sums_ref[k] = sums


def finish_kernel(pos_ref, stats_ref, win_ref, other_ref, per_dp_ref, hidden_ref, gamma_ref, beta_ref, loss_ref):
    dp = lax.axis_index('dp')
    total = functools.reduce(jnp.add, [per_dp_ref[k] for k in range(per_dp_ref.shape[0])])
    lines = total.shape[0] // 2
    gamma_ref[...] = jnp.concatenate([total[n:n + 1, :] for n in range(lines)], axis=1)
    beta_ref[...] = jnp.concatenate([total[n:n + 1, :] for n in range(lines, 2 * lines)], axis=1)
    loss_ref[...] = stats_ref[4:5, 0:1]
    lower = win_ref.shape[0]
    slot = pos_ref[0:1, :] - lax.rem(dp, 2) * lower
    slot = jnp.where(slot < 0, slot + 2 * lower, slot)
    slot = jnp.where(pos_ref[0:1, :] < 0, -1, slot)
    up = lax.broadcasted_iota(jnp.int32, (lower, slot.shape[1]), 0)
    out = jnp.zeros(hidden_ref.shape, jnp.float32)
    for part, ref in enumerate((win_ref, other_ref)):
        pick = jnp.where(up + part * lower == slot, 1.0, 0.0).astype(jnp.bfloat16)
        out = out + dot(pick, ref[...].astype(jnp.bfloat16), ((0,), (0,)))
    hidden_ref[...] = out.astype(jnp.bfloat16)


VMEM = pl.BlockSpec(memory_space=pltpu.VMEM)
ANY = pl.BlockSpec(memory_space=pl.ANY)


def solution(mesh):
    n_tp, n_dp = mesh.shape['tp'], mesh.shape['dp']

    def local_step(hidden, ln_gamma, ln_beta, embed, labels, loss_mask):
        tp, dp = lax.axis_index('tp'), lax.axis_index('dp')
        rows, width = embed.shape
        half = rows // 2
        tile = 1120 if half % 1120 == 0 and half > 1120 else half // 14
        tiles = half // tile
        x, c = dp // 2, dp % 2
        f32, bf16 = jnp.float32, jnp.bfloat16

        e_half, zc, zt, hw, wmask, stats, pos = pl.pallas_call(
            functools.partial(front_kernel, n_tp, rows, tile),
            out_shape=(pltpu.VMEM((half, width), bf16), jax.ShapeDtypeStruct((4 * SEQ, width), bf16), jax.ShapeDtypeStruct((width, 4 * SEQ), bf16),
                       jax.ShapeDtypeStruct((BLOCK, width), bf16), jax.ShapeDtypeStruct((BLOCK, 128), f32),
                       jax.ShapeDtypeStruct((8, 4 * SEQ), f32), jax.ShapeDtypeStruct((8, SEQ), jnp.int32)),
            in_specs=[ANY] * 6,
            out_specs=[VMEM] * 7,
            scratch_shapes=[
                pltpu.VMEM((SEQ, width), bf16), pltpu.VMEM((1, width), f32), pltpu.VMEM((1, width), f32),
                pltpu.VMEM((1, SEQ), jnp.int32), pltpu.VMEM((1, SEQ), jnp.int32),
                pltpu.VMEM((4, SEQ + 8, width), f32), pltpu.VMEM((4 * SEQ, width), bf16), pltpu.VMEM((BLOCK, width), bf16),
                pltpu.VMEM((tile, BLOCK), f32), pltpu.VMEM((4 * n_tp, 2, BLOCK), f32),
                pltpu.SemaphoreType.DMA((5,)), pltpu.SemaphoreType.DMA((tiles,)), pltpu.SemaphoreType.DMA((3,)), pltpu.SemaphoreType.DMA((3,)),
                pltpu.SemaphoreType.DMA((4 * n_tp,)), pltpu.SemaphoreType.DMA((4 * n_tp,)),
            ],
            compiler_params=pltpu.CompilerParams(collective_id=0, has_side_effects=True, vmem_limit_bytes=12 << 20),
            cost_estimate=pl.CostEstimate(flops=2 * half * BLOCK * width, bytes_accessed=2 * half * width, transcendentals=0),
        )(*[pltpu.with_memory_space_constraint(v, pltpu.HBM) for v in (hidden[0], ln_gamma[None], ln_beta[None], labels, loss_mask, embed)])

        def back(resident, source, spans, d_embed=None):
            slots = 2 if resident else 3
            scratch = [pltpu.VMEM((tile, 2 * BLOCK), f32), pltpu.VMEM((2 * tile if resident else tile, 2 * BLOCK), bf16),
                       pltpu.VMEM((slots, tile, width), f32), pltpu.SemaphoreType.DMA((slots,))]
            ops, specs = [source, zc, zt, stats], [VMEM if resident else ANY, VMEM, VMEM, VMEM]
            shapes, outs, alias = [jax.ShapeDtypeStruct((rows, width), f32)], [ANY], {}
            if resident:
                shapes.append(jax.ShapeDtypeStruct((BLOCK, width), f32))
                outs.append(VMEM)
            else:
                ops.append(d_embed)
                specs.append(ANY)
                alias = {4: 0}
                scratch += [pltpu.VMEM((IN_SLOTS, tile, width), bf16), pltpu.SemaphoreType.DMA((IN_SLOTS,)), pltpu.SemaphoreType.DMA((5,))]
            n = spans[0][1] - spans[0][0]
            return pl.pallas_call(
                functools.partial(back_kernel, tile, resident, slots, spans), out_shape=shapes, in_specs=specs, out_specs=outs,
                scratch_shapes=scratch, input_output_aliases=alias,
                compiler_params=pltpu.CompilerParams(vmem_limit_bytes=(19 if resident else 34) << 20, has_side_effects=True),
                cost_estimate=pl.CostEstimate(flops=6 * n * tile * BLOCK * width, bytes_accessed=6 * n * tile * width, transcendentals=0),
            )(*ops)

        d_embed, dz = back(True, e_half, ((0, tiles),) * 2)

        def small(body, out_shape, *ops):
            return pl.pallas_call(
                body, out_shape=out_shape, in_specs=[VMEM] * len(ops), out_specs=jax.tree.map(lambda _: VMEM, out_shape),
                compiler_params=pltpu.CompilerParams(vmem_limit_bytes=8 << 20),
                cost_estimate=pl.CostEstimate(flops=1 << 20, bytes_accessed=1 << 20, transcendentals=0),
            )(*ops)

        def shape(*dims):
            return jax.ShapeDtypeStruct(dims, f32)

        even = tiles // 4 * 2

        lower = BLOCK // 2
        share = lower // n_tp
        swap = [(0, 1), (1, 0), (2, 3), (3, 2)]
        arrived = lax.ppermute(lax.dynamic_slice_in_dim(dz, (1 - c) * lower, lower, 0), 'dp', swap)
        dz_half = small(add_kernel, shape(lower, width), dz, arrived)
        got = lax.all_to_all(dz_half.reshape(n_tp, share, width), 'tp', 0, 0)
        d_embed, dz_half = lax.optimization_barrier((d_embed, dz_half))
        (d_embed,) = back(False, embed, ((0, tiles // 2), (0, even)), d_embed)
        d_embed, got = lax.optimization_barrier((d_embed, got))

        packets = small(norm_kernel, shape(n_tp, share, width + 128), hw, wmask, ln_gamma[None], ln_beta[None], got)
        packed = lax.all_to_all(packets, 'tp', 0, 0)
        d_embed, packets = lax.optimization_barrier((d_embed, packets))
        (d_embed,) = back(False, embed, ((tiles // 2, tiles), (even, tiles)), d_embed)
        d_embed, packed = lax.optimization_barrier((d_embed, packed))

        d_win, sums = small(order_kernel, [shape(lower, width), shape(n_dp, width // 64, 128)], packed)
        other = lax.ppermute(d_win, 'dp', swap)
        per_dp = lax.all_to_all(sums, 'dp', 0, 0)
        d_hidden, d_gamma, d_beta, loss = small(
            finish_kernel, [jax.ShapeDtypeStruct((SEQ, width), bf16), shape(1, width), shape(1, width), shape(1, 1)],
            pos, stats, d_win, other, per_dp)
        return loss[0, 0], d_hidden[None], d_embed, d_gamma[0], d_beta[0]

    return jax.shard_map(local_step, mesh=mesh, in_specs=(P('dp', None, None), P(None), P(None), P('tp', None), P('dp', None), P('dp', None)), out_specs=(P(), P('dp', None, None), P('tp', None), P(None), P(None)), check_vma=False)
```

```python
import functools

import jax
import jax.numpy as jnp
from jax import lax
from jax.experimental import pallas as pl
from jax.experimental.pallas import tpu as pltpu
from jax.sharding import PartitionSpec as P

MESH = pl.DeviceIdType.MESH
LAYER_EPS = 1e-5
SEQ = 128
BLOCK = 256
IN_SLOTS = 5


def dot(a, b, contract, precision=None):
    return lax.dot_general(a, b, ((contract[0], contract[1]), ((), ())), precision=precision, preferred_element_type=jnp.float32)


def layer_norm(h, gamma, beta):
    centered = h - jnp.mean(h, axis=-1, keepdims=True)
    inv_std = lax.rsqrt(jnp.mean(centered * centered, axis=-1, keepdims=True) + LAYER_EPS)
    x_hat = centered * inv_std
    return x_hat, inv_std, (x_hat * gamma + beta).astype(jnp.bfloat16)


def front_kernel(n_tp, rows, tile, hid_in, gamma_in, beta_in, lab_in, mask_in, embed_ref,
                 half_ref, zc_ref, zt_ref, hw_ref, wmask_ref, stats_ref, pos_ref,
                 hid_ref, gamma_ref, beta_ref, lab_ref, mask_ref, hx, z_all, h_chip, logit, st, in_sem, e_sem, x_send, x_recv, st_send, st_recv):
    tp, dp = lax.axis_index('tp'), lax.axis_index('dp')
    n_dev = n_tp * 4
    me = tp * 4 + dp
    x, c = dp // 2, dp % 2
    sib, far = x * 2 + (1 - c), (1 - x) * 2 + c
    far_sib = (1 - x) * 2 + (1 - c)
    half = rows // 2
    tiles = half // tile
    width = hid_ref.shape[1]
    pairs = ((hid_in, hid_ref), (gamma_in, gamma_ref), (beta_in, beta_ref), (lab_in, lab_ref), (mask_in, mask_ref))
    loads = [pltpu.make_async_copy(a, b, in_sem.at[k]) for k, (a, b) in enumerate(pairs)]
    for load in loads:
        load.start()

    def fetch(i):
        return pltpu.make_async_copy(
            embed_ref.at[pl.ds(pl.multiple_of(c * half + i * tile, 16), tile)],
            half_ref.at[pl.ds(pl.multiple_of(i * tile, 16), tile)], e_sem.at[i])

    def start_fetch(i, carry):
        fetch(i).start()
        return carry

    lax.fori_loop(0, min(IN_SLOTS - 1, tiles), start_fetch, 0)

    barrier = pltpu.get_barrier_semaphore()

    peers = [(dt, dd) for dt in reversed(range(n_tp)) for dd in range(4) if dt or dd]

    def peer(dt, dd):
        return lax.rem(tp + dt, n_tp), lax.rem(dp + dd, 4)

    for dt, dd in peers:
        pl.semaphore_signal(barrier, inc=1, device_id=peer(dt, dd), device_id_type=MESH)

    for load in loads:
        load.wait()
    lab = jnp.broadcast_to(lab_ref[...].astype(jnp.float32), (8, SEQ))
    msk = jnp.broadcast_to(mask_ref[...].astype(jnp.float32), (8, SEQ))
    hx[dp, pl.ds(SEQ, 8), :] = jnp.concatenate([lab, msk, jnp.zeros((8, width - 2 * SEQ), jnp.float32)], axis=1)

    def widen(r, carry):
        at = pl.ds(pl.multiple_of(r * 32, 32), 32)
        hx[dp, at, :] = hid_ref[at, :].astype(jnp.float32)
        return carry

    lax.fori_loop(0, SEQ // 32, widen, 0)

    def norm(slot):
        def chunk(r, carry):
            at = pl.multiple_of(r * 32, 32)
            h = hx[slot, pl.ds(at, 32), :]
            z_all[pl.ds(pl.multiple_of(slot * SEQ + at, 32), 32), :] = layer_norm(h, gamma_ref[...], beta_ref[...])[2]
            return carry
        lax.fori_loop(0, SEQ // 32, chunk, 0)

    def chip_rows(slot, place):
        def chunk(r, carry):
            at = pl.multiple_of(r * 32, 32)
            h_chip[pl.ds(pl.multiple_of(place * SEQ + at, 32), 32), :] = hx[slot, pl.ds(at, 32), :].astype(jnp.bfloat16)
            return carry
        lax.fori_loop(0, SEQ // 32, chunk, 0)

    pl.semaphore_wait(barrier, n_dev - 1)

    def send(slot, k, to):
        return pltpu.make_async_remote_copy(
            src_ref=hx.at[slot], dst_ref=hx.at[slot], send_sem=x_send.at[k], recv_sem=x_recv.at[k],
            device_id=(tp, to), device_id_type=MESH)

    to_sib, to_far = send(dp, 0, sib), send(dp, 1, far)
    to_sib.start()
    to_far.start()
    norm(dp)
    chip_rows(dp, c)
    send(sib, 0, sib).wait_recv()
    norm(sib)
    chip_rows(sib, 1 - c)

    def labels_of(slot):
        return hx[slot, pl.ds(SEQ, 1), pl.ds(0, SEQ)]

    chip_lab = jnp.concatenate([labels_of(2 * x), labels_of(2 * x + 1)], axis=1).astype(jnp.int32)
    first_row = tp * rows + c * half
    chip_tokens = pl.ds(pl.multiple_of(x * BLOCK, BLOCK), BLOCK)
    piece = tile // 14 if tile % (14 * 8) == 0 else tile

    def product(i):
        logit[...] = dot(half_ref[pl.ds(pl.multiple_of(i * tile, 16), tile), :], z_all[chip_tokens, :], ((1,), (1,)))

    fetch(0).wait()
    product(0)
    row_iota = lax.broadcasted_iota(jnp.int32, (piece, BLOCK), 0)

    def absorb(i, carry, last=False):
        top, total, target = carry

        if not last:
            @pl.when(i + IN_SLOTS - 1 < tiles)
            def _():
                fetch(i + IN_SLOTS - 1).start()

            fetch(i + 1).wait()

        new_top = top
        for r in range(0, tile, piece):
            v = logit[pl.ds(r, piece), :].reshape(piece // 8, 8, BLOCK)
            new_top = jnp.maximum(new_top, jnp.max(v, axis=0))
        total = total * jnp.exp(top - new_top)
        lab_here = chip_lab - (first_row + i * tile)
        for r in range(0, tile, piece):
            v = logit[pl.ds(r, piece), :]
            e = jnp.exp(v.reshape(piece // 8, 8, BLOCK) - new_top[None])
            total = total + jnp.sum(e, axis=0)
            hit = jnp.where(row_iota == lab_here - r, v, 0.0)
            target = target + jnp.sum(hit.reshape(piece // 8, 8, BLOCK), axis=0)
        if not last:
            product(i + 1)
        return new_top, total, target

    zero = jnp.zeros((8, BLOCK), jnp.float32)
    carry = lax.fori_loop(0, tiles - 1, absorb, (jnp.full((8, BLOCK), -jnp.inf, jnp.float32), zero, zero))
    top, total, target = absorb(tiles - 1, carry, last=True)

    best = jnp.max(top, axis=0, keepdims=True)
    part = best + jnp.log(jnp.sum(total * jnp.exp(top - best), axis=0, keepdims=True))
    st[me, pl.ds(0, 1), :] = part
    st[me, pl.ds(1, 1), :] = jnp.sum(target, axis=0, keepdims=True)

    def stat(dt, dd, incoming):
        to = peer(dt, dd)
        owner = to[0] * 4 + to[1] if incoming else me
        return pltpu.make_async_remote_copy(
            src_ref=st.at[me], dst_ref=st.at[owner], send_sem=st_send.at[dt * 4 + dd], recv_sem=st_recv.at[owner],
            device_id=to, device_id_type=MESH)

    for dt, dd in peers:
        stat(dt, dd, False).start()

    send(far, 1, far).wait_recv()
    to_sib2 = send(far, 2, sib)
    to_sib2.start()
    norm(far)
    send(far_sib, 2, sib).wait_recv()
    norm(far_sib)

    lab_all = jnp.concatenate([labels_of(s) for s in range(4)], axis=1)
    mask_all = jnp.concatenate([hx[s, pl.ds(SEQ, 1), pl.ds(SEQ, SEQ)] for s in range(4)], axis=1)
    n_tok = 4 * SEQ
    lane = lax.broadcasted_iota(jnp.int32, (1, n_tok), 1)
    up = lax.broadcasted_iota(jnp.int32, (n_tok, n_tok), 0)
    across = lax.broadcasted_iota(jnp.int32, (n_tok, n_tok), 1)
    before = jnp.where((up < across) & (up // BLOCK == across // BLOCK), 1.0, 0.0).astype(jnp.bfloat16)
    rank = dot(jnp.broadcast_to(mask_all, (8, n_tok)).astype(jnp.bfloat16), before, ((1,), (0,)))[0:1, :]
    count_0 = jnp.sum(mask_all[:, :BLOCK], axis=1, keepdims=True)
    count_1 = jnp.sum(mask_all[:, BLOCK:], axis=1, keepdims=True)
    count = count_0 + count_1
    one_block = count <= BLOCK
    base_1 = jnp.where(one_block, BLOCK, 2 * BLOCK) - count_1
    col = jnp.where(lane < BLOCK, rank, rank + base_1)
    col = jnp.where(mask_all > 0.0, col, -1.0).astype(jnp.int32)
    chosen = up == col
    packing = jnp.where(chosen, 1.0, 0.0)
    packing_16 = packing.astype(jnp.bfloat16)
    zc_ref[...] = dot(packing_16, z_all[...], ((1,), (0,))).astype(jnp.bfloat16)
    zt_ref[...] = dot(z_all[...], packing_16, ((0,), (1,))).astype(jnp.bfloat16)

    window = jnp.where(one_block, 0, x * BLOCK)
    mine = jnp.where(x == 0, col[:, :BLOCK], col[:, BLOCK:]) - window
    w_pack = jnp.where(lax.broadcasted_iota(jnp.int32, (BLOCK, BLOCK), 0) == mine, 1.0, 0.0)
    hw_ref[...] = dot(w_pack.astype(jnp.bfloat16), h_chip[...], ((1,), (0,))).astype(jnp.bfloat16)
    wmask_ref[...] = jnp.broadcast_to(jnp.sum(w_pack, axis=1, keepdims=True), (BLOCK, 128))
    own = jnp.where(c == 0, mine[:, :SEQ], mine[:, SEQ:])
    pos_ref[...] = jnp.broadcast_to(own, (8, SEQ))

    to_sib.wait_send()
    to_far.wait_send()
    to_sib2.wait_send()
    for dt, dd in peers:
        stat(dt, dd, False).wait_send()
    for dt, dd in peers:
        stat(dt, dd, True).wait_recv()
    lse, goal = [], []
    for group in range(2):
        ids = [t * 4 + 2 * group + k for t in range(n_tp) for k in range(2)]
        parts = [st[d, pl.ds(0, 1), :] for d in ids]
        m = functools.reduce(jnp.maximum, parts)
        lse.append(m + jnp.log(sum(jnp.exp(p - m) for p in parts)))
        goal.append(sum(st[d, pl.ds(1, 1), :] for d in ids))
    lse, goal = jnp.concatenate(lse, axis=1), jnp.concatenate(goal, axis=1)
    loss = jnp.sum(mask_all * (lse - goal), axis=1, keepdims=True) / count

    values = jnp.concatenate([lse, lab_all, jnp.ones((6, n_tok), jnp.float32)], axis=0)
    packed = dot(values, packing, ((1,), (1,)), lax.Precision.HIGHEST)
    used = jnp.sum(jnp.where(packed[2:3, :] > 0.5, 1.0, 0.0), axis=0, keepdims=True)
    stats_ref[pl.ds(0, 1), :] = jnp.where(used > 0.5, packed[0:1, :], 1e30)
    stats_ref[pl.ds(1, 1), :] = jnp.where(used > 0.5, packed[1:2, :], -1.0)
    stats_ref[pl.ds(2, 1), :] = jnp.broadcast_to(1.0 / count, (1, n_tok))
    stats_ref[pl.ds(3, 1), :] = jnp.broadcast_to(count, (1, n_tok))
    stats_ref[pl.ds(4, 1), :] = jnp.broadcast_to(loss, (1, n_tok))
    stats_ref[pl.ds(5, 3), :] = jnp.zeros((3, n_tok), jnp.float32)


def back_kernel(tile, resident, slots, spans, *refs):
    if resident:
        embed_ref, zc_ref, zt_ref, stats_ref, out_ref, dz_ref, logit, grad, staged, out_sem = refs
    else:
        embed_ref, zc_ref, zt_ref, stats_ref, _, out_ref, logit, grad, staged, out_sem, held, in_sem = refs
    tp, dp = lax.axis_index('tp'), lax.axis_index('dp')
    chip, c = dp // 2, dp % 2
    rows = out_ref.shape[0]
    vocab_0, row_0 = tp * rows, (c if resident else 1 - c) * (rows // 2)
    count = jnp.max(stats_ref[pl.ds(3, 1), :])
    chunk = tile // 5 if tile % (5 * 16) == 0 else tile
    piece = chunk // 2 if chunk % 32 == 0 else chunk
    width = zc_ref.shape[1]

    def fetch(i):
        slot = lax.rem(i, IN_SLOTS)
        return pltpu.make_async_copy(embed_ref.at[pl.ds(pl.multiple_of(row_0 + i * tile, 16), tile)], held.at[slot], in_sem.at[slot])

    def rows_of(i, r, n):
        if resident:
            return embed_ref[pl.ds(pl.multiple_of(i * tile + r, 16), n), :]
        return held[lax.rem(i, IN_SLOTS), pl.ds(r, n), :]

    def put(i):
        slot = lax.rem(i, slots)
        return pltpu.make_async_copy(staged.at[slot], out_ref.at[pl.ds(pl.multiple_of(row_0 + i * tile, 16), tile)], out_sem.at[slot])

    def put_piece(i, q):
        slot = lax.rem(i, slots)
        return pltpu.make_async_copy(
            staged.at[slot, pl.ds(q, chunk)], out_ref.at[pl.ds(pl.multiple_of(row_0 + i * tile + q, 16), chunk)], out_sem.at[slot])

    def run(blocks):
        cols = blocks * BLOCK
        t_0, t_1 = spans[blocks - 1]
        unroll = 2 if resident or blocks == 2 else 1
        lse = stats_ref[pl.ds(0, 1), pl.ds(0, cols)]
        label = stats_ref[pl.ds(1, 1), pl.ds(0, cols)].astype(jnp.int32) - (vocab_0 + row_0)
        scale = stats_ref[pl.ds(2, 1), pl.ds(0, cols)]
        row_iota = lax.broadcasted_iota(jnp.int32, (piece, cols), 0)

        def product(i, r):
            logit[pl.ds(r, chunk), pl.ds(0, cols)] = dot(rows_of(i, r, chunk), zt_ref[:, pl.ds(0, cols)], ((1,), (0,)))

        if not resident:
            for k in range(min(IN_SLOTS - 1, t_1 - t_0)):
                fetch(t_0 + k).start()
            fetch(t_0).wait()
        else:
            dz_ref[...] = jnp.zeros_like(dz_ref)
        for r in range(0, tile, chunk):
            product(t_0, r)

        def stage(i, slot, base, last):
            later = jnp.minimum(i + 1, t_1 - 1)
            if not resident and not last:
                @pl.when(i + IN_SLOTS - 1 < t_1)
                def _():
                    fetch(i + IN_SLOTS - 1).start()

                @pl.when(i + 1 < t_1)
                def _():
                    fetch(i + 1).wait()

            @pl.when(i - slots >= t_0)
            def _():
                put(i - slots).wait()

            here = label - i * tile
            for q in range(0, tile, chunk):
                for r in range(q, q + chunk, piece):
                    p = jnp.exp(logit[pl.ds(r, piece), pl.ds(0, cols)] - lse)
                    g = jnp.where(row_iota == here - r, p - 1.0, p) * scale
                    grad[pl.ds(base + r, piece), pl.ds(0, cols)] = g.astype(jnp.bfloat16)
                if not last:
                    product(later, q)
                staged[slot, pl.ds(q, chunk), :] = dot(grad[pl.ds(base + q, chunk), pl.ds(0, cols)], zc_ref[pl.ds(0, cols), :], ((1,), (0,)))
                put_piece(i, q).start()

        def body(p, carry):
            i = t_0 + unroll * p
            for u in range(unroll):
                slot = u if resident else lax.rem(i + u, slots)
                stage(i + u, slot, u * tile if resident else 0, False)
            if resident:
                window = grad[:, pl.ds(0, BLOCK)]
                if blocks > 1:
                    window = jnp.where(chip == 0, window, grad[:, pl.ds(BLOCK, BLOCK)])
                for n in range(0, width, 256):
                    dz_ref[:, pl.ds(n, 256)] += dot(window, rows_of(i, 0, 2 * tile)[:, n:n + 256], ((0,), (0,)))
            return carry

        trips = (t_1 - t_0) // unroll
        lax.fori_loop(0, trips, body, 0)
        if trips * unroll < t_1 - t_0:
            stage(t_1 - 1, (t_1 - 1) % slots, 0, True)

        def drain(i, carry):
            put(i).wait()
            return carry

        lax.fori_loop(max(t_0, t_1 - slots), t_1, drain, 0)

    @pl.when(count <= BLOCK)
    def _():
        run(1)

    @pl.when(count > BLOCK)
    def _():
        run(2)


def add_kernel(dz_ref, arrived_ref, out_ref):
    lower = out_ref.shape[0]
    at = pl.multiple_of(lax.rem(lax.axis_index('dp'), 2) * lower, 8)
    out_ref[...] = dz_ref[pl.ds(at, lower), :] + arrived_ref[...]


def norm_kernel(hw_ref, wmask_ref, gamma_ref, beta_ref, got_ref, packet_ref):
    n_tp, share, width = got_ref.shape
    dz = functools.reduce(jnp.add, [got_ref[k] for k in range(n_tp)])
    at = pl.multiple_of(lax.rem(lax.axis_index('dp'), 2) * (n_tp * share) + lax.axis_index('tp') * share, 8)
    gamma = gamma_ref[...]
    x_hat, inv_std, _ = layer_norm(hw_ref[pl.ds(at, share), :].astype(jnp.float32), gamma, beta_ref[...])
    scaled = dz * gamma
    d_h = (scaled - jnp.mean(scaled, axis=-1, keepdims=True) - x_hat * jnp.mean(scaled * x_hat, axis=-1, keepdims=True)) * inv_std
    kept = dz * wmask_ref[pl.ds(at, share), pl.ds(0, 1)]
    d_gamma = jnp.sum(kept * x_hat, axis=0, keepdims=True)
    d_beta = jnp.sum(kept, axis=0, keepdims=True)
    sums = jnp.concatenate([v[:, n:n + 128] for v in (d_gamma, d_beta) for n in range(0, width, 128)], axis=0)
    for k in range(n_tp):
        packet_ref[k, :, pl.ds(0, width)] = d_h
        packet_ref[k, pl.ds(0, sums.shape[0]), pl.ds(width, 128)] = sums


def order_kernel(packets_ref, win_ref, sums_ref):
    n_tp, share = packets_ref.shape[:2]
    width = win_ref.shape[1]
    for k in range(n_tp):
        win_ref[pl.ds(k * share, share), :] = packets_ref[k, :, pl.ds(0, width)]
    sums_ref[...] = functools.reduce(jnp.add, [packets_ref[k, pl.ds(0, width // 64), pl.ds(width, 128)] for k in range(n_tp)])


def finish_kernel(pos_ref, stats_ref, win_ref, other_ref, *refs):
    per_dp, (hidden_ref, gamma_ref, beta_ref, loss_ref) = refs[:4], refs[4:]
    dp = lax.axis_index('dp')
    total = jnp.zeros_like(per_dp[0])
    for owner in range(4):
        term = per_dp[0][...]
        for k in range(1, 4):
            term = jnp.where(lax.rem(dp + k, 4) == owner, per_dp[k][...], term)
        total = total + term
    lines = total.shape[0] // 2
    gamma_ref[...] = jnp.concatenate([total[n:n + 1, :] for n in range(lines)], axis=1)
    beta_ref[...] = jnp.concatenate([total[n:n + 1, :] for n in range(lines, 2 * lines)], axis=1)
    loss_ref[...] = stats_ref[4:5, 0:1]
    lower = win_ref.shape[0]
    slot = pos_ref[0:1, :] - lax.rem(dp, 2) * lower
    slot = jnp.where(slot < 0, slot + 2 * lower, slot)
    slot = jnp.where(pos_ref[0:1, :] < 0, -1, slot)
    up = lax.broadcasted_iota(jnp.int32, (lower, slot.shape[1]), 0)
    out = jnp.zeros(hidden_ref.shape, jnp.float32)
    for part, ref in enumerate((win_ref, other_ref)):
        pick = jnp.where(up + part * lower == slot, 1.0, 0.0).astype(jnp.bfloat16)
        out = out + dot(pick, ref[...].astype(jnp.bfloat16), ((0,), (0,)))
    hidden_ref[...] = out.astype(jnp.bfloat16)


VMEM = pl.BlockSpec(memory_space=pltpu.VMEM)
ANY = pl.BlockSpec(memory_space=pl.ANY)


def solution(mesh):
    n_tp, n_dp = mesh.shape['tp'], mesh.shape['dp']

    def local_step(hidden, ln_gamma, ln_beta, embed, labels, loss_mask):
        tp, dp = lax.axis_index('tp'), lax.axis_index('dp')
        rows, width = embed.shape
        half = rows // 2
        tile = 1120 if half % 1120 == 0 and half > 1120 else half // 14
        tiles = half // tile
        x, c = dp // 2, dp % 2
        f32, bf16 = jnp.float32, jnp.bfloat16

        e_half, zc, zt, hw, wmask, stats, pos = pl.pallas_call(
            functools.partial(front_kernel, n_tp, rows, tile),
            out_shape=(pltpu.VMEM((half, width), bf16), jax.ShapeDtypeStruct((4 * SEQ, width), bf16), jax.ShapeDtypeStruct((width, 4 * SEQ), bf16),
                       jax.ShapeDtypeStruct((BLOCK, width), bf16), jax.ShapeDtypeStruct((BLOCK, 128), f32),
                       jax.ShapeDtypeStruct((8, 4 * SEQ), f32), jax.ShapeDtypeStruct((8, SEQ), jnp.int32)),
            in_specs=[ANY] * 6,
            out_specs=[VMEM] * 7,
            scratch_shapes=[
                pltpu.VMEM((SEQ, width), bf16), pltpu.VMEM((1, width), f32), pltpu.VMEM((1, width), f32),
                pltpu.VMEM((1, SEQ), jnp.int32), pltpu.VMEM((1, SEQ), jnp.int32),
                pltpu.VMEM((4, SEQ + 8, width), f32), pltpu.VMEM((4 * SEQ, width), bf16), pltpu.VMEM((BLOCK, width), bf16),
                pltpu.VMEM((tile, BLOCK), f32), pltpu.VMEM((4 * n_tp, 2, BLOCK), f32),
                pltpu.SemaphoreType.DMA((5,)), pltpu.SemaphoreType.DMA((tiles,)), pltpu.SemaphoreType.DMA((3,)), pltpu.SemaphoreType.DMA((3,)),
                pltpu.SemaphoreType.DMA((4 * n_tp,)), pltpu.SemaphoreType.DMA((4 * n_tp,)),
            ],
            compiler_params=pltpu.CompilerParams(collective_id=0, has_side_effects=True, vmem_limit_bytes=12 << 20),
            cost_estimate=pl.CostEstimate(flops=2 * half * BLOCK * width, bytes_accessed=2 * half * width, transcendentals=0),
        )(*[pltpu.with_memory_space_constraint(v, pltpu.HBM) for v in (hidden[0], ln_gamma[None], ln_beta[None], labels, loss_mask, embed)])

        def back(resident, source, spans, d_embed=None):
            slots = 2 if resident else 3
            scratch = [pltpu.VMEM((tile, 2 * BLOCK), f32), pltpu.VMEM((2 * tile if resident else tile, 2 * BLOCK), bf16),
                       pltpu.VMEM((slots, tile, width), f32), pltpu.SemaphoreType.DMA((slots,))]
            ops, specs = [source, zc, zt, stats], [VMEM if resident else ANY, VMEM, VMEM, VMEM]
            shapes, outs, alias = [jax.ShapeDtypeStruct((rows, width), f32)], [ANY], {}
            if resident:
                shapes.append(jax.ShapeDtypeStruct((BLOCK, width), f32))
                outs.append(VMEM)
            else:
                ops.append(d_embed)
                specs.append(ANY)
                alias = {4: 0}
                scratch += [pltpu.VMEM((IN_SLOTS, tile, width), bf16), pltpu.SemaphoreType.DMA((IN_SLOTS,))]
            n = spans[0][1] - spans[0][0]
            return pl.pallas_call(
                functools.partial(back_kernel, tile, resident, slots, spans), out_shape=shapes, in_specs=specs, out_specs=outs,
                scratch_shapes=scratch, input_output_aliases=alias,
                compiler_params=pltpu.CompilerParams(vmem_limit_bytes=(19 if resident else 34) << 20, has_side_effects=True),
                cost_estimate=pl.CostEstimate(flops=6 * n * tile * BLOCK * width, bytes_accessed=6 * n * tile * width, transcendentals=0),
            )(*ops)

        d_embed, dz = back(True, e_half, ((0, tiles),) * 2)

        def small(body, out_shape, *ops):
            return pl.pallas_call(
                body, out_shape=out_shape, in_specs=[VMEM] * len(ops), out_specs=jax.tree.map(lambda _: VMEM, out_shape),
                compiler_params=pltpu.CompilerParams(vmem_limit_bytes=8 << 20),
                cost_estimate=pl.CostEstimate(flops=1 << 20, bytes_accessed=1 << 20, transcendentals=0),
            )(*ops)

        def shape(*dims):
            return jax.ShapeDtypeStruct(dims, f32)

        lower = BLOCK // 2
        share = lower // n_tp
        swap = [(0, 1), (1, 0), (2, 3), (3, 2)]
        arrived = lax.ppermute(lax.dynamic_slice_in_dim(dz, (1 - c) * lower, lower, 0), 'dp', swap)
        dz_half = small(add_kernel, shape(lower, width), dz, arrived)
        got = lax.all_to_all(dz_half.reshape(n_tp, share, width), 'tp', 0, 0)
        d_embed, dz_half = lax.optimization_barrier((d_embed, dz_half))
        (d_embed,) = back(False, embed, ((0, tiles // 2),) * 2, d_embed)
        d_embed, got = lax.optimization_barrier((d_embed, got))

        packets = small(norm_kernel, shape(n_tp, share, width + 128), hw, wmask, ln_gamma[None], ln_beta[None], got)
        packed = lax.all_to_all(packets, 'tp', 0, 0)
        d_embed, packets = lax.optimization_barrier((d_embed, packets))
        (d_embed,) = back(False, embed, ((tiles // 2, tiles),) * 2, d_embed)
        d_embed, packed = lax.optimization_barrier((d_embed, packed))

        d_win, sums = small(order_kernel, [shape(lower, width), shape(width // 64, 128)], packed)
        other = lax.ppermute(d_win, 'dp', swap)
        per_dp = [sums] + [lax.ppermute(sums, 'dp', [(i, (i - k) % n_dp) for i in range(n_dp)]) for k in range(1, n_dp)]
        d_hidden, d_gamma, d_beta, loss = small(
            finish_kernel, [jax.ShapeDtypeStruct((SEQ, width), bf16), shape(1, width), shape(1, width), shape(1, 1)],
            pos, stats, d_win, other, *per_dp)
        return loss[0, 0], d_hidden[None], d_embed, d_gamma[0], d_beta[0]

    return jax.shard_map(local_step, mesh=mesh, in_specs=(P('dp', None, None), P(None), P(None), P('tp', None), P('dp', None), P('dp', None)), out_specs=(P(), P('dp', None, None), P('tp', None), P(None), P(None)), check_vma=False)
```
